32 devices in a mesh: row: 8 (over z, y), col: 2 (over core), depth: 2 (over x).
Axes of the slice: x: 2, y: 2, z: 4, core: 2. Of those that a mesh axis runs over, the one named last changes fastest.
Arguments:
- student_hidden: bfloat16 [2048, 768], P('row', ('depth', 'col')), may hold values from -16 to 16
- embedding: bfloat16 [50304, 768], P('col', ('depth', 'row')), as said below
- teacher_logits: bfloat16 [2048, 50304], P('row', ('col', 'depth')), may hold values from -24 to 124, as said below
Outputs:
- loss: float32 [2048], P('row')
- peak_logprob: float32 [2048], P('row')
The draws below stay inside these ranges and needn't reach their ends.
Inputs may be any that keep to these rules, and one draw needn't show every extreme that they name: embedding entries lie within plus or minus 4 / sqrt(768). teacher_logits lie within -24 and 124; each token's logits carry an offset of 0 to 100.
All inputs are finite; a program needn't handle non-finite values.
Results may differ from the reference program's by a relative error of at most 0.0003.
Values may be sent and summed in bfloat16 or wider, within the bound.
A program may use at most 128 MiB of HBM per device.

```python
import jax
import jax.numpy as jnp
from jax import lax

D = 768
VOCAB = 50304
TOK_DEV = 256
TOKENS = 2048
N_ROW = 8


def embedding_table(key):
    base = jax.random.normal(jax.random.fold_in(key, 101), (VOCAB, D), jnp.float32)
    return jnp.clip(base, -4.0, 4.0) * D ** (-0.5)


def draw_embedding(key, part):
    return embedding_table(key).astype(jnp.bfloat16)


def draw_student_hidden(key, part):
    hidden = jnp.clip(jax.random.normal(jax.random.fold_in(key, 205), (TOKENS, D), jnp.float32), -6.0, 6.0)
    return jnp.clip(hidden, -16.0, 16.0).astype(jnp.bfloat16)


def draw_teacher_logits(key, part):
    offsets = jax.random.uniform(jax.random.fold_in(key, 301), (TOKENS, 1), jnp.float32, 0.0, 100.0)
    noise = 4.0 * jnp.clip(jax.random.normal(jax.random.fold_in(key, 304), (TOKENS, VOCAB), jnp.float32), -6.0, 6.0)
    return (offsets + noise).astype(jnp.bfloat16)


def setup_inputs(seed: int = 0) -> dict:
    streams_of = jax.random.split(jax.random.key(seed), 4)
    student_hidden = draw_student_hidden(jax.random.fold_in(streams_of[3], 71), 0)
    embedding = draw_embedding(jax.random.fold_in(streams_of[3], 71), 0)
    teacher_logits = draw_teacher_logits(jax.random.fold_in(streams_of[3], 71), 0)
    return {"student_hidden": student_hidden, "embedding": embedding, "teacher_logits": teacher_logits}


def reference(student_hidden, embedding, teacher_logits):
    def token_block(pair):
        hidden_rows, teacher_rows = pair
        student = jnp.dot(hidden_rows, embedding.T, preferred_element_type=jnp.float32)
        teacher_values = teacher_rows.astype(jnp.float32)
        student_peak = jnp.max(student, axis=1)
        teacher_peak = jnp.max(teacher_values, axis=1)
        student_sum = jnp.sum(jnp.exp(student - student_peak[:, None]), axis=1)
        weights = jnp.exp(teacher_values - teacher_peak[:, None])
        teacher_sum = jnp.sum(weights, axis=1)
        cross_sum = jnp.sum(weights * student, axis=1)
        norm_log = jnp.log(student_sum)
        return student_peak + norm_log - cross_sum / teacher_sum, -norm_log

    losses, peaks = lax.map(token_block, (student_hidden.reshape(N_ROW, TOK_DEV, D), teacher_logits.reshape(N_ROW, TOK_DEV, VOCAB)))
    return losses.reshape(TOKENS), peaks.reshape(TOKENS)
```

```python
import functools

import jax
import jax.numpy as jnp
from jax import lax
from jax.experimental import pallas as pl
from jax.experimental.pallas import tpu as pltpu
from jax.sharding import PartitionSpec as P

MESH = pl.DeviceIdType.MESH
GROUP = 2
LANE = 128
CHUNK = 256
KEPT = 0.64
LOW = -1e30


class Layout:
    def __init__(self, vocab, depths):
        self.half = vocab // depths
        self.stride = vocab // LANE // (depths * GROUP) * LANE
        self.shift = self.half - GROUP * self.stride
        self.last = self.half - (GROUP - 1) * self.stride
        top = self.last + self.shift * (depths - 1)
        self.chunks = -(-top // CHUNK)
        self.width = self.chunks * CHUNK
        self.kept = round(self.chunks * KEPT)
        self.tail = self.stride * (depths * GROUP - 1) + (self.chunks - 1) * CHUNK
        self.edge = (self.chunks - 1) * CHUNK
        assert depths == 2 and self.edge < self.stride and 0 <= self.shift < CHUNK and self.shift % 16 == 0
        assert vocab - self.tail <= CHUNK


def place():
    r, c, d = lax.axis_index("row"), lax.axis_index("col"), lax.axis_index("depth")
    return r, c, d, r // GROUP, lax.rem(r, GROUP)


def ends(rows, q):
    steps = rows // GROUP
    low, high = q == 0, q == steps - 1
    return low | high, (q == 1) | (q == steps - 2), jnp.where(q * 2 < steps, GROUP, -GROUP)


def as_count(flag):
    return flag.astype(jnp.int32)


def loop(begin, stop, body):
    def step(i, _):
        body(i)
        return 0

    lax.fori_loop(begin, stop, step, 0)


def merge(parts):
    top, total, teacher_top, teacher_total, cross = parts
    peak = jnp.max(top, axis=0, keepdims=True)
    teacher_peak = jnp.max(teacher_top, axis=0, keepdims=True)
    scale = jnp.exp(teacher_top - teacher_peak)
    return [
        peak,
        jnp.sum(total * jnp.exp(top - peak), axis=0, keepdims=True),
        teacher_peak,
        jnp.sum(teacher_total * scale, axis=0, keepdims=True),
        jnp.sum(cross * scale, axis=0, keepdims=True),
    ]


def add_terms(full_ref, hid_ref, acc, n, lanes, teacher, valid=None):
    rows = full_ref[:, :, :, lanes].reshape(-1, CHUNK)
    hidden = hid_ref[n].reshape(rows.shape[0], -1)
    tokens = hidden.shape[1]
    student = lax.dot_general(rows, hidden, (((0,), (0,)), ((), ())), preferred_element_type=jnp.float32)
    teacher = teacher.astype(jnp.float32)
    if valid is not None:
        index = lax.broadcasted_iota(jnp.int32, student.shape, 0)
        keep = (index >= valid[0]) & (index < valid[1])
        student = jnp.where(keep, student, LOW)
        teacher = jnp.where(keep, teacher, LOW)
    student = student.reshape(CHUNK // 8, 8, tokens)
    teacher = teacher.reshape(CHUNK // 8, 8, tokens)
    top = jnp.maximum(acc[n, 0], jnp.max(student, axis=0))
    acc[n, 1] = acc[n, 1] * jnp.exp(acc[n, 0] - top) + jnp.sum(jnp.exp(student - top[None]), axis=0)
    acc[n, 0] = top
    teacher_top = jnp.maximum(acc[n, 2], jnp.max(teacher, axis=0))
    fade = jnp.exp(acc[n, 2] - teacher_top)
    weights = jnp.exp(teacher - teacher_top[None])
    acc[n, 3] = acc[n, 3] * fade + jnp.sum(weights, axis=0)
    acc[n, 4] = acc[n, 4] * fade + jnp.sum(weights * student, axis=0)
    acc[n, 2] = teacher_top


def kernel(
    rows, cols, depths, lay, emb_ref, tail_ref, teacher_ref, hidden_ref, loss_ref, peak_ref,
    full_ref, own_ref, other_ref, extra_ref, hid_ref, acc, stats_ref, held_ref,
    own_sem, first_send, first_recv, right_send, left_send, line_recv, teach_send, teach_recv, extra_send, extra_recv,
    hid_send, hid_recv, stats_send, stats_recv,
):
    r, c, d, q, j = place()
    steps = rows // GROUP
    count = depths * GROUP
    me = d * GROUP + j
    chunks, kept, edge = lay.chunks, lay.kept, lay.edge
    end, server, inward = ends(rows, q)
    pj = lax.rem(j + 1, GROUP)
    pr = q * GROUP + pj
    slice_ = d * cols + c
    peers = []
    for dj in range(GROUP):
        for dc in range(cols):
            for dd in range(depths):
                if dj or dc or dd:
                    peers.append((q * GROUP + lax.rem(j + dj, GROUP), lax.rem(c + dc, cols), lax.rem(d + dd, depths), dj))
    group = [(r, c, d, 0)] + peers
    near = len(peers)
    same = [(a, b, e) for a, b, e, dj in peers if dj == 0]

    def lanes(t):
        return pl.ds(pl.multiple_of(t * CHUNK, CHUNK), CHUNK)

    has_head = ~((d > 0) & (j == 0))
    peer_head = ~((d > 0) & (pj == 0))
    has_tail = (d == depths - 1) & (j == GROUP - 1)
    peer_tail = (d == depths - 1) & (pj == GROUP - 1)
    shift = lay.shift * (depths - 1)

    def source(part, at, size):
        begin = jnp.clip(lay.stride * part - lay.shift * d + at, 0, lay.half - size)
        return teacher_ref.at[pl.ds(pl.multiple_of(begin, 16), size)]

    own_body = pltpu.make_async_copy(source(j, shift, lay.last - shift), own_ref.at[pl.ds(shift, lay.last - shift)], own_sem.at[0])
    own_head = pltpu.make_async_copy(source(j, 0, shift), own_ref.at[pl.ds(0, shift)], own_sem.at[1])
    own_tail = pltpu.make_async_copy(source(j, lay.last, shift), own_ref.at[pl.ds(lay.last, shift)], own_sem.at[2])
    own_body.start()

    @pl.when(has_head)
    def _():
        own_head.start()

    @pl.when(has_tail)
    def _():
        own_tail.start()

    own_hid = pltpu.make_async_copy(hidden_ref, hid_ref.at[0, slice_], own_sem.at[3])
    own_hid.start()

    def piece(target, t):
        return emb_ref.at[:, pl.ds(pl.multiple_of(lay.stride * target + t * CHUNK, LANE), CHUNK)]

    own_piece = pltpu.make_async_copy(
        emb_ref.at[:, pl.ds(pl.multiple_of(lay.stride * me, LANE), edge)], full_ref.at[d, r, :, pl.ds(0, edge)], own_sem.at[4]
    )
    own_piece.start()

    def own_edge(source_ref):
        return pltpu.make_async_copy(source_ref, full_ref.at[d, r, :, pl.ds(edge, CHUNK)], own_sem.at[5])

    @pl.when(me < count - 1)
    def _():
        own_edge(piece(me, chunks - 1)).start()

    @pl.when(me == count - 1)
    def _():
        own_edge(tail_ref).start()

    barrier = pltpu.get_barrier_semaphore()

    def greet(row, col, depth):
        pl.semaphore_signal(barrier, inc=1, device_id=(row, col, depth), device_id_type=MESH)

    for a, b, e, _ in peers:
        greet(a, b, e)

    @pl.when(q + 1 < steps)
    def _():
        greet(r + GROUP, c, d)

    @pl.when(q > 0)
    def _():
        greet(r - GROUP, c, d)

    @pl.when(end)
    def _():
        for a, b, e, _ in peers:
            greet(a + inward, b, e)

    @pl.when(server)
    def _():
        for a, b, e, _ in peers:
            greet(a - inward, b, e)

    pl.semaphore_wait(barrier, near * (1 + as_count(end | server)) + as_count(q + 1 < steps) + as_count(q > 0))

    def first(t, off, source_ref):
        target = lax.rem(me + off, count)
        return pltpu.make_async_remote_copy(
            src_ref=source_ref, dst_ref=full_ref.at[d, r, :, lanes(t)], send_sem=first_send.at[0], recv_sem=first_recv.at[t],
            device_id=(q * GROUP + lax.rem(target, GROUP), c, target // GROUP), device_id_type=MESH,
        )

    def first_arrived(t):
        at = full_ref.at[0, pl.ds(0, count - 1), :, lanes(t)]
        return pltpu.make_async_remote_copy(
            src_ref=at, dst_ref=at, send_sem=first_send.at[0], recv_sem=first_recv.at[t], device_id=(pr, c, d), device_id_type=MESH,
        )

    def send_line(source_ref, dst_ref, block, t, right):
        sems = right_send if right else left_send
        return pltpu.make_async_remote_copy(
            src_ref=source_ref, dst_ref=dst_ref, send_sem=sems.at[block], recv_sem=line_recv.at[block, t],
            device_id=(r + GROUP if right else r - GROUP, c, d), device_id_type=MESH,
        )

    def block_at(block, at):
        return full_ref.at[:, pl.ds(pl.multiple_of(block * GROUP, GROUP), GROUP), :, at]

    def along(block, t, right):
        at = block_at(block, lanes(t))
        return send_line(at, at, block, t, right)

    def to_right(t):
        return (q + 1 < steps) & ((t < kept) | (q + 2 < steps))

    def to_left(t):
        return (q > 0) & ((t < kept) | (q > 1))

    def both(t, source_ref, dst_ref):
        @pl.when(to_right(t))
        def _():
            send_line(source_ref, dst_ref, q, t, True).start()

        @pl.when(to_left(t))
        def _():
            send_line(source_ref, dst_ref, q, t, False).start()

    def launch(t):
        for off in range(1, count):
            first(t, off, piece(lax.rem(me + off, count), t)).start()
        both(t, piece(me, t), full_ref.at[d, r, :, lanes(t)])

    loop(0, chunks - 1, launch)
    final = chunks - 1
    for off in range(count):
        target = lax.rem(me + off, count)

        def send(source_ref, off=off):
            if off:
                first(final, off, source_ref).start()
            else:
                both(final, source_ref, full_ref.at[d, r, :, lanes(final)])

        @pl.when(target < count - 1)
        def _():
            send(piece(target, final))

        @pl.when(target == count - 1)
        def _():
            send(tail_ref)

    def give(n, sem, a, b, e, source_ref):
        return pltpu.make_async_remote_copy(
            src_ref=source_ref, dst_ref=hid_ref.at[n, slice_], send_sem=hid_send.at[sem], recv_sem=hid_recv.at[sem],
            device_id=(a, b, e), device_id_type=MESH,
        )

    ways = len(same) + 1
    cross = [give(1, 0, pr, c, d, hidden_ref), None, give(3, 2 * ways, pr, c, d, hid_ref.at[2, slice_])]
    spread = [
        [
            give(n, n * ways + 1 + k, a, b, e, hidden_ref if n == 0 else hid_ref.at[n, slice_])
            for k, (a, b, e) in enumerate(same)
        ]
        for n in range(2 * GROUP)
    ]
    far_hid = give(2, 4 * ways, r + inward, c, d, hidden_ref)
    cross[0].start()
    for copy in spread[0]:
        copy.start()

    body = lay.last - edge

    def teach(t, size=CHUNK, at=0):
        where = pl.multiple_of(t * CHUNK, CHUNK) + at
        return pltpu.make_async_remote_copy(
            src_ref=source(pj, where, size), dst_ref=other_ref.at[pl.ds(where, size)],
            send_sem=teach_send.at[0], recv_sem=teach_recv.at[t], device_id=(pr, c, d), device_id_type=MESH,
        )

    def teach_edge(n, at, size):
        return pltpu.make_async_remote_copy(
            src_ref=source(pj, at, size), dst_ref=other_ref.at[pl.ds(at, size)],
            send_sem=teach_send.at[1 + n], recv_sem=teach_recv.at[chunks + n], device_id=(pr, c, d), device_id_type=MESH,
        )

    def teach_kept():
        teach(0, CHUNK - shift, shift).start()

        @pl.when(peer_head)
        def _():
            teach_edge(0, 0, shift).start()

        loop(1, kept, lambda t: teach(t).start())

    def teach_rest():
        loop(kept, final, lambda t: teach(t).start())
        teach(final, body).start()

        @pl.when(peer_tail)
        def _():
            teach_edge(1, lay.last, shift).start()

    @pl.when(end)
    def _():
        teach_rest()

    teach_kept()

    @pl.when(~end)
    def _():
        teach_rest()

    def teach_first_arrived():
        teach(0, CHUNK - shift, shift).wait_recv()

        @pl.when(has_head)
        def _():
            teach_edge(0, 0, shift).wait_recv()

    def teach_last_arrived():
        teach(final, body).wait_recv()

        @pl.when(has_tail)
        def _():
            teach_edge(1, lay.last, shift).wait_recv()

    def start_line(t):
        first_arrived(t).wait_recv()
        for off in range(1, count):
            sender = lax.rem(me + count - off, count)
            at = full_ref.at[sender // GROUP, q * GROUP + lax.rem(sender, GROUP), :, lanes(t)]
            both(t, at, at)

    loop(0, chunks, start_line)

    cross[0].wait_recv()
    for copy in spread[1]:
        copy.start()

    def extra(n, t, size=CHUNK):
        where = pl.multiple_of(t * CHUNK, CHUNK)
        return pltpu.make_async_remote_copy(
            src_ref=source(j, where, size) if n == 0 else other_ref.at[pl.ds(where, size)],
            dst_ref=extra_ref.at[n, pl.ds(pl.multiple_of(where - kept * CHUNK, CHUNK), size)],
            send_sem=extra_send.at[n], recv_sem=extra_recv.at[n, t - kept], device_id=(r + inward, c, d), device_id_type=MESH,
        )

    def extra_edge(n):
        at = lay.last - kept * CHUNK
        return pltpu.make_async_remote_copy(
            src_ref=source(j, lay.last, shift) if n == 0 else other_ref.at[pl.ds(lay.last, shift)],
            dst_ref=extra_ref.at[n, pl.ds(at, shift)],
            send_sem=extra_send.at[GROUP + n], recv_sem=extra_recv.at[n, chunks - kept],
            device_id=(r + inward, c, d), device_id_type=MESH,
        )

    @pl.when(end)
    def _():
        far_hid.start()

        def pass_on(t):
            teach(t).wait_recv()
            for n in range(GROUP):
                extra(n, t).start()

        loop(kept, final, pass_on)
        teach_last_arrived()
        for n in range(GROUP):
            extra(n, final, body).start()

        @pl.when(has_tail)
        def _():
            for n in range(GROUP):
                extra_edge(n).start()

    def hop(k, t):
        wanted = (t < kept) | ~end

        @pl.when((q - k >= 0) & wanted)
        def _():
            along(q - k, t, True).wait_recv()

            @pl.when(to_right(t))
            def _():
                along(q - k, t, True).start()

        @pl.when((q + k < steps) & wanted)
        def _():
            along(q + k, t, False).wait_recv()

            @pl.when(to_left(t))
            def _():
                along(q + k, t, False).start()

    far = jnp.maximum(q, steps - 1 - q)
    loop(1, far, lambda k: loop(0, chunks, lambda t: hop(k, t)))

    for n in range(2 * GROUP):
        for k in range(5):
            acc[n, k] = jnp.full(acc.shape[2:], LOW if k in (0, 2) else 0.0, jnp.float32)

    def main(t, valid=None):
        at = pl.ds(pl.multiple_of(t * CHUNK, CHUNK), CHUNK)
        for n, ref in enumerate((own_ref, other_ref)):
            add_terms(full_ref, hid_ref, acc, n, at, ref[at, :], valid)

    def more(t, valid=None):
        at = pl.ds(pl.multiple_of(t * CHUNK, CHUNK), CHUNK)
        from_ = pl.ds(pl.multiple_of((t - kept) * CHUNK, CHUNK), CHUNK)
        for n in range(GROUP):
            add_terms(full_ref, hid_ref, acc, GROUP + n, at, extra_ref[n, from_, :], valid)

    hop(far, 0)

    @pl.when(server)
    def _():
        far_hid.wait_recv()
        cross[2].start()
        for copy in spread[2]:
            copy.start()

    own_body.wait()

    @pl.when(has_head)
    def _():
        own_head.wait()

    @pl.when(has_tail)
    def _():
        own_tail.wait()

    own_hid.wait()
    own_piece.wait()
    own_edge(tail_ref).wait()
    for n in range(2):
        for copy in spread[n]:
            copy.wait_recv()
    teach_first_arrived()
    main(0, (jnp.where(has_head, 0, shift), CHUNK))

    def kept_chunk(t):
        hop(far, t)
        teach(t).wait_recv()
        main(t)

    half = kept // 2
    loop(1, half, kept_chunk)

    @pl.when(server)
    def _():
        cross[2].wait_recv()
        for copy in spread[3]:
            copy.start()

    loop(half, kept, kept_chunk)

    @pl.when(server)
    def _():
        for n in range(2, 4):
            for copy in spread[n]:
                copy.wait_recv()

    limit = (0, jnp.where(j == 0, lay.stride, lay.last + lay.shift * d) - edge)

    @pl.when(~end)
    def _():
        def rest_chunk(t):
            hop(far, t)

            @pl.when(server)
            def _():
                for n in range(GROUP):
                    extra(n, t).wait_recv()
                more(t)

            teach(t).wait_recv()
            main(t)

        loop(kept, final, rest_chunk)
        hop(far, final)

    def close(n):
        values = merge([acc[n, k] for k in range(5)])
        stats_ref[n] = jnp.concatenate(values + [values[0]] * 3, axis=0)

    def tell(n, a, b, e, source_set):
        return pltpu.make_async_remote_copy(
            src_ref=stats_ref.at[source_set], dst_ref=held_ref.at[n], send_sem=stats_send.at[n], recv_sem=stats_recv.at[n],
            device_id=(a, b, e), device_id_type=MESH,
        )

    copies = [tell(n, a, b, e, dj) for n, (a, b, e, dj) in enumerate(peers)]
    far_copies = [tell(near + n, a - inward, b, e, GROUP + dj) for n, (a, b, e, dj) in enumerate(group)]

    @pl.when(server)
    def _():
        for n in range(GROUP):
            extra(n, final, body).wait_recv()

        @pl.when(has_tail)
        def _():
            for n in range(GROUP):
                extra_edge(n).wait_recv()

        more(final, limit)
        for n in range(GROUP, 2 * GROUP):
            close(n)
        for copy in far_copies:
            copy.start()

    @pl.when(~end)
    def _():
        teach_last_arrived()
        main(final, limit)

    for n in range(GROUP):
        close(n)
    for copy in copies:
        copy.start()

    @pl.when(~end)
    def _():
        for n in range(len(group)):
            for k in range(5):
                held_ref[near + n, k] = jnp.full(held_ref.shape[2:], LOW if k in (0, 2) else 0.0, jnp.float32)

    def settle(block):
        def sent(right, size):
            at = block_at(block, pl.ds(0, size))
            send_line(at, at, block, 0, right).wait_send()

        @pl.when((block <= q) & (q + 2 < steps))
        def _():
            sent(True, lay.width)

        @pl.when((block <= q) & (q + 2 == steps))
        def _():
            sent(True, kept * CHUNK)

        @pl.when((block >= q) & (q > 1))
        def _():
            sent(False, lay.width)

        @pl.when((block >= q) & (q == 1))
        def _():
            sent(False, kept * CHUNK)

    loop(0, steps, settle)
    sent_pieces = full_ref.at[0, pl.ds(0, count - 1)]
    pltpu.make_async_remote_copy(
        src_ref=sent_pieces, dst_ref=sent_pieces, send_sem=first_send.at[0], recv_sem=first_recv.at[0],
        device_id=(pr, c, d), device_id_type=MESH,
    ).wait_send()
    cross[0].wait_send()
    for n in range(2):
        for copy in spread[n]:
            copy.wait_send()
    whole = other_ref.at[pl.ds(shift, lay.last - shift)]
    pltpu.make_async_remote_copy(
        src_ref=whole, dst_ref=whole, send_sem=teach_send.at[0], recv_sem=teach_recv.at[0], device_id=(pr, c, d), device_id_type=MESH,
    ).wait_send()

    @pl.when(peer_head)
    def _():
        teach_edge(0, 0, shift).wait_send()

    @pl.when(peer_tail)
    def _():
        teach_edge(1, lay.last, shift).wait_send()

    @pl.when(end)
    def _():
        far_hid.wait_send()
        part = other_ref.at[pl.ds(kept * CHUNK, lay.last - kept * CHUNK)]
        for n in range(GROUP):
            pltpu.make_async_remote_copy(
                src_ref=part, dst_ref=part, send_sem=extra_send.at[n], recv_sem=extra_recv.at[n, 0],
                device_id=(pr, c, d), device_id_type=MESH,
            ).wait_send()

        @pl.when(has_tail)
        def _():
            for n in range(GROUP):
                extra_edge(n).wait_send()

    @pl.when(server)
    def _():
        cross[2].wait_send()
        for n in range(2, 4):
            for copy in spread[n]:
                copy.wait_send()
        for copy in far_copies:
            copy.wait_send()

    for copy in copies:
        copy.wait()

    @pl.when(end)
    def _():
        for copy in far_copies:
            copy.wait_recv()

    blocks = [stats_ref[0]] + [held_ref[n] for n in range(near + len(group))]
    parts = [jnp.concatenate([block[k : k + 1] for block in blocks], axis=0) for k in range(5)]
    peak, total, _, teacher_total, cross_sum = merge(parts)
    norm_log = jnp.log(total)
    loss_ref[...] = peak + norm_log - cross_sum / teacher_total
    peak_ref[...] = -norm_log


def on_device(rows, cols, depths, student_hidden, embedding, teacher_logits):
    vocab, narrow = embedding.shape
    lay = Layout(vocab, depths)
    table = embedding.T
    tail = jnp.pad(embedding.T[:, lay.tail :], ((0, 0), (0, lay.tail + CHUNK - vocab)))
    hidden = student_hidden.T
    features, tokens = hidden.shape
    steps = rows // GROUP
    peers = GROUP * cols * depths - 1
    slots = 2 * GROUP * cols * depths - 1
    ways = cols * depths
    chunks = lay.chunks
    dma = pltpu.SemaphoreType.DMA
    any_space = pl.BlockSpec(memory_space=pl.ANY)
    vmem = pl.BlockSpec(memory_space=pltpu.VMEM)
    dtype = embedding.dtype
    loss, peak = pl.pallas_call(
        functools.partial(kernel, rows, cols, depths, lay),
        out_shape=(jax.ShapeDtypeStruct((1, tokens), jnp.float32),) * 2,
        in_specs=[any_space] * 4,
        out_specs=(vmem, vmem),
        scratch_shapes=[
            pltpu.VMEM((depths, rows, narrow, lay.width), dtype),
            pltpu.VMEM((lay.width, tokens), teacher_logits.dtype),
            pltpu.VMEM((lay.width, tokens), teacher_logits.dtype),
            pltpu.VMEM((GROUP, lay.width - lay.kept * CHUNK, tokens), teacher_logits.dtype),
            pltpu.VMEM((2 * GROUP, depths * cols, features, tokens), hidden.dtype),
            pltpu.VMEM((2 * GROUP, 5, 8, tokens), jnp.float32),
            pltpu.VMEM((2 * GROUP, 8, tokens), jnp.float32),
            pltpu.VMEM((slots, 8, tokens), jnp.float32),
            dma((6,)), dma((1,)), dma((chunks,)), dma((steps,)), dma((steps,)), dma((steps, chunks)),
            dma((3,)), dma((chunks + 2,)), dma((2 * GROUP,)), dma((GROUP, chunks - lay.kept + 1)),
            dma((4 * ways + 1,)), dma((4 * ways + 1,)), dma((slots,)), dma((slots,)),
        ],
        compiler_params=pltpu.CompilerParams(collective_id=0, has_side_effects=True, vmem_limit_bytes=60 * 2**20),
        name="distill",
    )(table, tail, teacher_logits.T, hidden)
    return loss.reshape(-1), peak.reshape(-1)


def solution(mesh):
    sizes = [mesh.shape[name] for name in ("row", "col", "depth")]
    in_specs = (P("row", ("depth", "col")), P("col", ("depth", "row")), P("row", ("col", "depth")))
    out_specs = (P("row"), P("row"))
    return jax.shard_map(
        functools.partial(on_device, *sizes), mesh=mesh, in_specs=in_specs, out_specs=out_specs, check_vma=False
    )
```

```python
import functools

import jax
import jax.numpy as jnp
from jax import lax
from jax.experimental import pallas as pl
from jax.experimental.pallas import tpu as pltpu
from jax.sharding import PartitionSpec as P

MESH = pl.DeviceIdType.MESH
GROUP = 2
LANE = 128
CHUNK = 256
KEPT = 0.64
LOW = -1e30


class Layout:
    def __init__(self, vocab, depths):
        self.half = vocab // depths
        self.stride = vocab // LANE // (depths * GROUP) * LANE
        self.shift = self.half - GROUP * self.stride
        self.last = self.half - (GROUP - 1) * self.stride
        top = self.last + self.shift * (depths - 1)
        self.chunks = -(-top // CHUNK)
        self.width = self.chunks * CHUNK
        self.kept = round(self.chunks * KEPT)
        self.tail = self.stride * (depths * GROUP - 1) + (self.chunks - 1) * CHUNK
        self.edge = (self.chunks - 1) * CHUNK
        assert depths == 2 and self.edge < self.stride and 0 <= self.shift < CHUNK and self.shift % 16 == 0
        assert vocab - self.tail <= CHUNK


def place():
    r, c, d = lax.axis_index("row"), lax.axis_index("col"), lax.axis_index("depth")
    return r, c, d, r // GROUP, lax.rem(r, GROUP)


def ends(rows, q):
    steps = rows // GROUP
    low, high = q == 0, q == steps - 1
    return low | high, (q == 1) | (q == steps - 2), jnp.where(q * 2 < steps, GROUP, -GROUP)


def as_count(flag):
    return flag.astype(jnp.int32)


def loop(begin, stop, body):
    def step(i, _):
        body(i)
        return 0

    lax.fori_loop(begin, stop, step, 0)


def merge(parts):
    top, total, teacher_top, teacher_total, cross = parts
    peak = jnp.max(top, axis=0, keepdims=True)
    teacher_peak = jnp.max(teacher_top, axis=0, keepdims=True)
    scale = jnp.exp(teacher_top - teacher_peak)
    return [
        peak,
        jnp.sum(total * jnp.exp(top - peak), axis=0, keepdims=True),
        teacher_peak,
        jnp.sum(teacher_total * scale, axis=0, keepdims=True),
        jnp.sum(cross * scale, axis=0, keepdims=True),
    ]


def add_terms(full_ref, hid_ref, acc, n, lanes, teacher, valid=None):
    rows = full_ref[:, :, :, lanes].reshape(-1, CHUNK)
    hidden = hid_ref[n].reshape(rows.shape[0], -1)
    tokens = hidden.shape[1]
    student = lax.dot_general(rows, hidden, (((0,), (0,)), ((), ())), preferred_element_type=jnp.float32)
    teacher = teacher.astype(jnp.float32)
    if valid is not None:
        index = lax.broadcasted_iota(jnp.int32, student.shape, 0)
        keep = (index >= valid[0]) & (index < valid[1])
        student = jnp.where(keep, student, LOW)
        teacher = jnp.where(keep, teacher, LOW)
    student = student.reshape(CHUNK // 8, 8, tokens)
    teacher = teacher.reshape(CHUNK // 8, 8, tokens)
    top = jnp.maximum(acc[n, 0], jnp.max(student, axis=0))
    acc[n, 1] = acc[n, 1] * jnp.exp(acc[n, 0] - top) + jnp.sum(jnp.exp(student - top[None]), axis=0)
    acc[n, 0] = top
    teacher_top = jnp.maximum(acc[n, 2], jnp.max(teacher, axis=0))
    fade = jnp.exp(acc[n, 2] - teacher_top)
    weights = jnp.exp(teacher - teacher_top[None])
    acc[n, 3] = acc[n, 3] * fade + jnp.sum(weights, axis=0)
    acc[n, 4] = acc[n, 4] * fade + jnp.sum(weights * student, axis=0)
    acc[n, 2] = teacher_top


def kernel(
    rows, cols, depths, lay, emb_ref, teacher_ref, hidden_ref, sums_ref,
    table_ref, tail_ref, full_ref, own_ref, other_ref, extra_ref, hid_ref, acc, stats_ref, held_ref,
    own_sem, first_send, first_recv, right_send, left_send, line_recv, teach_send, teach_recv, extra_send, extra_recv,
    hid_send, hid_recv, stats_send, stats_recv,
):
    r, c, d, q, j = place()
    steps = rows // GROUP
    count = depths * GROUP
    me = d * GROUP + j
    chunks, kept, edge = lay.chunks, lay.kept, lay.edge
    end, server, inward = ends(rows, q)
    pj = lax.rem(j + 1, GROUP)
    pr = q * GROUP + pj
    slice_ = d * cols + c
    peers = []
    for dj in range(GROUP):
        for dc in range(cols):
            for dd in range(depths):
                if dj or dc or dd:
                    peers.append((q * GROUP + lax.rem(j + dj, GROUP), lax.rem(c + dc, cols), lax.rem(d + dd, depths), dj))
    group = [(r, c, d, 0)] + peers
    near = len(peers)
    same = [(a, b, e) for a, b, e, dj in peers if dj == 0]

    def lanes(t):
        return pl.ds(pl.multiple_of(t * CHUNK, CHUNK), CHUNK)

    barrier = pltpu.get_barrier_semaphore()

    def greet(row, col, depth):
        pl.semaphore_signal(barrier, inc=1, device_id=(row, col, depth), device_id_type=MESH)

    for a, b, e, _ in peers:
        greet(a, b, e)

    @pl.when(q + 1 < steps)
    def _():
        greet(r + GROUP, c, d)

    @pl.when(q > 0)
    def _():
        greet(r - GROUP, c, d)

    has_head = ~((d > 0) & (j == 0))
    peer_head = ~((d > 0) & (pj == 0))
    has_tail = (d == depths - 1) & (j == GROUP - 1)
    peer_tail = (d == depths - 1) & (pj == GROUP - 1)
    shift = lay.shift * (depths - 1)

    def source(part, at, size):
        begin = jnp.clip(lay.stride * part - lay.shift * d + at, 0, lay.half - size)
        return teacher_ref.at[pl.ds(pl.multiple_of(begin, 16), size)]

    own_body = pltpu.make_async_copy(source(j, shift, lay.last - shift), own_ref.at[pl.ds(shift, lay.last - shift)], own_sem.at[0])
    own_head = pltpu.make_async_copy(source(j, 0, shift), own_ref.at[pl.ds(0, shift)], own_sem.at[1])
    own_tail = pltpu.make_async_copy(source(j, lay.last, shift), own_ref.at[pl.ds(lay.last, shift)], own_sem.at[2])
    load = pltpu.make_async_copy(emb_ref, table_ref, own_sem.at[6])
    load.start()
    own_body.start()

    @pl.when(has_head)
    def _():
        own_head.start()

    @pl.when(has_tail)
    def _():
        own_tail.start()

    own_hid = pltpu.make_async_copy(hidden_ref, hid_ref.at[0, slice_], own_sem.at[3])
    own_hid.start()

    def piece(target, t):
        return table_ref.at[:, pl.ds(pl.multiple_of(lay.stride * target + t * CHUNK, LANE), CHUNK)]

    own_piece = pltpu.make_async_copy(
        table_ref.at[:, pl.ds(pl.multiple_of(lay.stride * me, LANE), edge)], full_ref.at[d, r, :, pl.ds(0, edge)], own_sem.at[4]
    )

    def own_edge(source_ref):
        return pltpu.make_async_copy(source_ref, full_ref.at[d, r, :, pl.ds(edge, CHUNK)], own_sem.at[5])

    load.wait()
    left = table_ref.shape[1] - lay.tail
    tail_ref[:, :left] = table_ref[:, lay.tail :]
    tail_ref[:, left:] = jnp.zeros((tail_ref.shape[0], CHUNK - left), tail_ref.dtype)
    own_piece.start()

    @pl.when(me < count - 1)
    def _():
        own_edge(piece(me, chunks - 1)).start()

    @pl.when(me == count - 1)
    def _():
        own_edge(tail_ref).start()

    pl.semaphore_wait(barrier, near + as_count(q + 1 < steps) + as_count(q > 0))

    def first(t, off, source_ref):
        target = lax.rem(me + off, count)
        return pltpu.make_async_remote_copy(
            src_ref=source_ref, dst_ref=full_ref.at[d, r, :, lanes(t)], send_sem=first_send.at[0], recv_sem=first_recv.at[t],
            device_id=(q * GROUP + lax.rem(target, GROUP), c, target // GROUP), device_id_type=MESH,
        )

    def first_arrived(t):
        at = full_ref.at[0, pl.ds(0, count - 1), :, lanes(t)]
        return pltpu.make_async_remote_copy(
            src_ref=at, dst_ref=at, send_sem=first_send.at[0], recv_sem=first_recv.at[t], device_id=(pr, c, d), device_id_type=MESH,
        )

    def send_line(source_ref, dst_ref, block, t, right):
        sems = right_send if right else left_send
        return pltpu.make_async_remote_copy(
            src_ref=source_ref, dst_ref=dst_ref, send_sem=sems.at[block], recv_sem=line_recv.at[block, t],
            device_id=(r + GROUP if right else r - GROUP, c, d), device_id_type=MESH,
        )

    def block_at(block, at):
        return full_ref.at[:, pl.ds(pl.multiple_of(block * GROUP, GROUP), GROUP), :, at]

    def along(block, t, right):
        at = block_at(block, lanes(t))
        return send_line(at, at, block, t, right)

    def to_right(t):
        return (q + 1 < steps) & ((t < kept) | (q + 2 < steps))

    def to_left(t):
        return (q > 0) & ((t < kept) | (q > 1))

    def both(t, source_ref, dst_ref):
        @pl.when(to_right(t))
        def _():
            send_line(source_ref, dst_ref, q, t, True).start()

        @pl.when(to_left(t))
        def _():
            send_line(source_ref, dst_ref, q, t, False).start()

    def give(n, sem, a, b, e, source_ref):
        return pltpu.make_async_remote_copy(
            src_ref=source_ref, dst_ref=hid_ref.at[n, slice_], send_sem=hid_send.at[sem], recv_sem=hid_recv.at[sem],
            device_id=(a, b, e), device_id_type=MESH,
        )

    ways = len(same) + 1
    cross = [give(1, 0, pr, c, d, hidden_ref), None, give(3, 2 * ways, pr, c, d, hid_ref.at[2, slice_])]
    spread = [
        [
            give(n, n * ways + 1 + k, a, b, e, hidden_ref if n == 0 else hid_ref.at[n, slice_])
            for k, (a, b, e) in enumerate(same)
        ]
        for n in range(2 * GROUP)
    ]
    far_hid = give(2, 4 * ways, r + inward, c, d, hidden_ref)
    @pl.when(end)
    def _():
        far_hid.start()

    def launch(t):
        for off in range(1, count):
            first(t, off, piece(lax.rem(me + off, count), t)).start()
        both(t, piece(me, t), full_ref.at[d, r, :, lanes(t)])

    loop(0, chunks - 1, launch)
    final = chunks - 1
    for off in range(count):
        target = lax.rem(me + off, count)

        def send(source_ref, off=off):
            if off:
                first(final, off, source_ref).start()
            else:
                both(final, source_ref, full_ref.at[d, r, :, lanes(final)])

        @pl.when(target < count - 1)
        def _():
            send(piece(target, final))

        @pl.when(target == count - 1)
        def _():
            send(tail_ref)

    cross[0].start()
    for copy in spread[0]:
        copy.start()

    @pl.when(server)
    def _():
        far_hid.wait_recv()
        cross[2].start()
        for copy in spread[2]:
            copy.start()

    body = lay.last - edge

    def teach(t, size=CHUNK, at=0):
        where = pl.multiple_of(t * CHUNK, CHUNK) + at
        return pltpu.make_async_remote_copy(
            src_ref=source(pj, where, size), dst_ref=other_ref.at[pl.ds(where, size)],
            send_sem=teach_send.at[0], recv_sem=teach_recv.at[t], device_id=(pr, c, d), device_id_type=MESH,
        )

    def teach_edge(n, at, size):
        return pltpu.make_async_remote_copy(
            src_ref=source(pj, at, size), dst_ref=other_ref.at[pl.ds(at, size)],
            send_sem=teach_send.at[1 + n], recv_sem=teach_recv.at[chunks + n], device_id=(pr, c, d), device_id_type=MESH,
        )

    def teach_kept():
        teach(0, CHUNK - shift, shift).start()

        @pl.when(peer_head)
        def _():
            teach_edge(0, 0, shift).start()

        loop(1, kept, lambda t: teach(t).start())

    def teach_rest():
        loop(kept, final, lambda t: teach(t).start())
        teach(final, body).start()

        @pl.when(peer_tail)
        def _():
            teach_edge(1, lay.last, shift).start()

    def teach_first_arrived():
        teach(0, CHUNK - shift, shift).wait_recv()

        @pl.when(has_head)
        def _():
            teach_edge(0, 0, shift).wait_recv()

    def teach_last_arrived():
        teach(final, body).wait_recv()

        @pl.when(has_tail)
        def _():
            teach_edge(1, lay.last, shift).wait_recv()

    def start_line(t):
        first_arrived(t).wait_recv()
        for off in range(1, count):
            sender = lax.rem(me + count - off, count)
            at = full_ref.at[sender // GROUP, q * GROUP + lax.rem(sender, GROUP), :, lanes(t)]
            both(t, at, at)

    loop(0, chunks, start_line)

    @pl.when(end)
    def _():
        teach_rest()

    teach_kept()

    @pl.when(~end)
    def _():
        teach_rest()

    cross[0].wait_recv()
    for copy in spread[1]:
        copy.start()

    @pl.when(server)
    def _():
        cross[2].wait_recv()
        for copy in spread[3]:
            copy.start()

    def extra(n, t, size=CHUNK):
        where = pl.multiple_of(t * CHUNK, CHUNK)
        return pltpu.make_async_remote_copy(
            src_ref=source(j, where, size) if n == 0 else other_ref.at[pl.ds(where, size)],
            dst_ref=extra_ref.at[n, pl.ds(pl.multiple_of(where - kept * CHUNK, CHUNK), size)],
            send_sem=extra_send.at[n], recv_sem=extra_recv.at[n, t - kept], device_id=(r + inward, c, d), device_id_type=MESH,
        )

    def extra_edge(n):
        at = lay.last - kept * CHUNK
        return pltpu.make_async_remote_copy(
            src_ref=source(j, lay.last, shift) if n == 0 else other_ref.at[pl.ds(lay.last, shift)],
            dst_ref=extra_ref.at[n, pl.ds(at, shift)],
            send_sem=extra_send.at[GROUP + n], recv_sem=extra_recv.at[n, chunks - kept],
            device_id=(r + inward, c, d), device_id_type=MESH,
        )

    @pl.when(end)
    def _():
        def pass_on(t):
            teach(t).wait_recv()
            for n in range(GROUP):
                extra(n, t).start()

        loop(kept, final, pass_on)
        teach_last_arrived()
        for n in range(GROUP):
            extra(n, final, body).start()

        @pl.when(has_tail)
        def _():
            for n in range(GROUP):
                extra_edge(n).start()

    def hop(k, t):
        wanted = (t < kept) | ~end

        @pl.when((q - k >= 0) & wanted)
        def _():
            along(q - k, t, True).wait_recv()

            @pl.when(to_right(t))
            def _():
                along(q - k, t, True).start()

        @pl.when((q + k < steps) & wanted)
        def _():
            along(q + k, t, False).wait_recv()

            @pl.when(to_left(t))
            def _():
                along(q + k, t, False).start()

    far = jnp.maximum(q, steps - 1 - q)
    loop(1, far, lambda k: loop(0, chunks, lambda t: hop(k, t)))

    for n in range(2 * GROUP):
        for k in range(5):
            acc[n, k] = jnp.full(acc.shape[2:], LOW if k in (0, 2) else 0.0, jnp.float32)

    def main(t, valid=None):
        at = pl.ds(pl.multiple_of(t * CHUNK, CHUNK), CHUNK)
        for n, ref in enumerate((own_ref, other_ref)):
            add_terms(full_ref, hid_ref, acc, n, at, ref[at, :], valid)

    def more(t, valid=None):
        at = pl.ds(pl.multiple_of(t * CHUNK, CHUNK), CHUNK)
        from_ = pl.ds(pl.multiple_of((t - kept) * CHUNK, CHUNK), CHUNK)
        for n in range(GROUP):
            add_terms(full_ref, hid_ref, acc, GROUP + n, at, extra_ref[n, from_, :], valid)

    hop(far, 0)
    own_body.wait()

    @pl.when(has_head)
    def _():
        own_head.wait()

    @pl.when(has_tail)
    def _():
        own_tail.wait()

    own_hid.wait()
    own_piece.wait()
    own_edge(tail_ref).wait()
    for n in range(2):
        for copy in spread[n]:
            copy.wait_recv()
    teach_first_arrived()
    main(0, (jnp.where(has_head, 0, shift), CHUNK))

    def kept_chunk(t):
        hop(far, t)
        teach(t).wait_recv()
        main(t)

    loop(1, kept, kept_chunk)

    @pl.when(server)
    def _():
        for n in range(2, 4):
            for copy in spread[n]:
                copy.wait_recv()

    limit = (0, jnp.where(j == 0, lay.stride, lay.last + lay.shift * d) - edge)

    @pl.when(~end)
    def _():
        def rest_chunk(t):
            hop(far, t)

            @pl.when(server)
            def _():
                for n in range(GROUP):
                    extra(n, t).wait_recv()
                more(t)

            teach(t).wait_recv()
            main(t)

        loop(kept, final, rest_chunk)
        hop(far, final)

    def close(n):
        values = merge([acc[n, k] for k in range(5)])
        stats_ref[n] = jnp.concatenate(values + [values[0]] * 3, axis=0)

    def tell(n, a, b, e, source_set):
        return pltpu.make_async_remote_copy(
            src_ref=stats_ref.at[source_set], dst_ref=held_ref.at[n], send_sem=stats_send.at[n], recv_sem=stats_recv.at[n],
            device_id=(a, b, e), device_id_type=MESH,
        )

    copies = [tell(n, a, b, e, dj) for n, (a, b, e, dj) in enumerate(peers)]
    far_copies = [tell(near + n, a - inward, b, e, GROUP + dj) for n, (a, b, e, dj) in enumerate(group)]

    @pl.when(server)
    def _():
        for n in range(GROUP):
            extra(n, final, body).wait_recv()

        @pl.when(has_tail)
        def _():
            for n in range(GROUP):
                extra_edge(n).wait_recv()

        more(final, limit)
        for n in range(GROUP, 2 * GROUP):
            close(n)
        for copy in far_copies:
            copy.start()

    @pl.when(~end)
    def _():
        teach_last_arrived()
        main(final, limit)

    for n in range(GROUP):
        close(n)
    for copy in copies:
        copy.start()

    @pl.when(~end)
    def _():
        for n in range(len(group)):
            for k in range(5):
                held_ref[near + n, k] = jnp.full(held_ref.shape[2:], LOW if k in (0, 2) else 0.0, jnp.float32)

    def settle(block):
        def sent(right, size):
            at = block_at(block, pl.ds(0, size))
            send_line(at, at, block, 0, right).wait_send()

        @pl.when((block <= q) & (q + 2 < steps))
        def _():
            sent(True, lay.width)

        @pl.when((block <= q) & (q + 2 == steps))
        def _():
            sent(True, kept * CHUNK)

        @pl.when((block >= q) & (q > 1))
        def _():
            sent(False, lay.width)

        @pl.when((block >= q) & (q == 1))
        def _():
            sent(False, kept * CHUNK)

    loop(0, steps, settle)
    sent_pieces = full_ref.at[0, pl.ds(0, count - 1)]
    pltpu.make_async_remote_copy(
        src_ref=sent_pieces, dst_ref=sent_pieces, send_sem=first_send.at[0], recv_sem=first_recv.at[0],
        device_id=(pr, c, d), device_id_type=MESH,
    ).wait_send()
    cross[0].wait_send()
    for n in range(2):
        for copy in spread[n]:
            copy.wait_send()
    whole = other_ref.at[pl.ds(shift, lay.last - shift)]
    pltpu.make_async_remote_copy(
        src_ref=whole, dst_ref=whole, send_sem=teach_send.at[0], recv_sem=teach_recv.at[0], device_id=(pr, c, d), device_id_type=MESH,
    ).wait_send()

    @pl.when(peer_head)
    def _():
        teach_edge(0, 0, shift).wait_send()

    @pl.when(peer_tail)
    def _():
        teach_edge(1, lay.last, shift).wait_send()

    @pl.when(end)
    def _():
        far_hid.wait_send()
        part = other_ref.at[pl.ds(kept * CHUNK, lay.last - kept * CHUNK)]
        for n in range(GROUP):
            pltpu.make_async_remote_copy(
                src_ref=part, dst_ref=part, send_sem=extra_send.at[n], recv_sem=extra_recv.at[n, 0],
                device_id=(pr, c, d), device_id_type=MESH,
            ).wait_send()

        @pl.when(has_tail)
        def _():
            for n in range(GROUP):
                extra_edge(n).wait_send()

    @pl.when(server)
    def _():
        cross[2].wait_send()
        for n in range(2, 4):
            for copy in spread[n]:
                copy.wait_send()
        for copy in far_copies:
            copy.wait_send()

    for copy in copies:
        copy.wait()

    @pl.when(end)
    def _():
        for copy in far_copies:
            copy.wait_recv()

    blocks = [stats_ref[0]] + [held_ref[n] for n in range(near + len(group))]
    parts = [jnp.concatenate([block[k : k + 1] for block in blocks], axis=0) for k in range(5)]
    peak, total, _, teacher_total, cross_sum = merge(parts)
    sums_ref[...] = jnp.concatenate([peak, total, teacher_total, cross_sum] + [peak] * 4, axis=0)


def on_device(rows, cols, depths, student_hidden, embedding, teacher_logits):
    vocab, narrow = embedding.shape
    lay = Layout(vocab, depths)
    hidden = student_hidden.T
    features, tokens = hidden.shape
    steps = rows // GROUP
    peers = GROUP * cols * depths - 1
    slots = 2 * GROUP * cols * depths - 1
    ways = cols * depths
    chunks = lay.chunks
    dma = pltpu.SemaphoreType.DMA
    any_space = pl.BlockSpec(memory_space=pl.ANY)
    vmem = pl.BlockSpec(memory_space=pltpu.VMEM)
    dtype = embedding.dtype
    sums = pl.pallas_call(
        functools.partial(kernel, rows, cols, depths, lay),
        out_shape=jax.ShapeDtypeStruct((8, tokens), jnp.float32),
        in_specs=[any_space] * 3,
        out_specs=vmem,
        scratch_shapes=[
            pltpu.VMEM((narrow, vocab), dtype),
            pltpu.VMEM((narrow, CHUNK), dtype),
            pltpu.VMEM((depths, rows, narrow, lay.width), dtype),
            pltpu.VMEM((lay.width, tokens), teacher_logits.dtype),
            pltpu.VMEM((lay.width, tokens), teacher_logits.dtype),
            pltpu.VMEM((GROUP, lay.width - lay.kept * CHUNK, tokens), teacher_logits.dtype),
            pltpu.VMEM((2 * GROUP, depths * cols, features, tokens), hidden.dtype),
            pltpu.VMEM((2 * GROUP, 5, 8, tokens), jnp.float32),
            pltpu.VMEM((2 * GROUP, 8, tokens), jnp.float32),
            pltpu.VMEM((slots, 8, tokens), jnp.float32),
            dma((7,)), dma((1,)), dma((chunks,)), dma((steps,)), dma((steps,)), dma((steps, chunks)),
            dma((3,)), dma((chunks + 2,)), dma((2 * GROUP,)), dma((GROUP, chunks - lay.kept + 1)),
            dma((4 * ways + 1,)), dma((4 * ways + 1,)), dma((slots,)), dma((slots,)),
        ],
        compiler_params=pltpu.CompilerParams(collective_id=0, has_side_effects=True, vmem_limit_bytes=60 * 2**20),
        name="distill",
    )(embedding.T, teacher_logits.T, hidden)
    norm_log = jnp.log(sums[1])
    return sums[0] + norm_log - sums[3] / sums[2], -norm_log


def solution(mesh):
    sizes = [mesh.shape[name] for name in ("row", "col", "depth")]
    in_specs = (P("row", ("depth", "col")), P("col", ("depth", "row")), P("row", ("col", "depth")))
    out_specs = (P("row"), P("row"))
    return jax.shard_map(
        functools.partial(on_device, *sizes), mesh=mesh, in_specs=in_specs, out_specs=out_specs, check_vma=False
    )
```

```python
import functools

import jax
import jax.numpy as jnp
from jax import lax
from jax.experimental import pallas as pl
from jax.experimental.pallas import tpu as pltpu
from jax.sharding import PartitionSpec as P

MESH = pl.DeviceIdType.MESH
GROUP = 2
LANE = 128
CHUNK = 512
KEPT = 0.64
LOW = -1e30


class Layout:
    def __init__(self, vocab, depths):
        self.half = vocab // depths
        self.stride = vocab // LANE // (depths * GROUP) * LANE
        self.shift = self.half - GROUP * self.stride
        self.last = self.half - (GROUP - 1) * self.stride
        self.edge = (self.stride - LANE) // CHUNK * CHUNK
        self.whole = self.edge // CHUNK
        self.plain = self.stride - self.edge
        self.rest = self.plain + LANE // 2
        self.kept = round(self.stride / CHUNK * KEPT)
        assert depths == 2 and 0 <= self.shift < CHUNK and self.shift % 16 == 0
        assert self.last + self.shift <= self.stride + LANE // 2 and self.plain % LANE == 0
        assert vocab <= self.stride * depths * GROUP + LANE // 2


def place():
    r, c, d = lax.axis_index("row"), lax.axis_index("col"), lax.axis_index("depth")
    return r, c, d, r // GROUP, lax.rem(r, GROUP)


def ends(rows, q):
    steps = rows // GROUP
    low, high = q == 0, q == steps - 1
    return low | high, (q == 1) | (q == steps - 2), jnp.where(q * 2 < steps, GROUP, -GROUP)


def as_count(flag):
    return flag.astype(jnp.int32)


def loop(begin, stop, body):
    def step(i, _):
        body(i)
        return 0

    lax.fori_loop(begin, stop, step, 0)


def merge(parts):
    top, total, teacher_top, teacher_total, cross = parts
    peak = jnp.max(top, axis=0, keepdims=True)
    teacher_peak = jnp.max(teacher_top, axis=0, keepdims=True)
    scale = jnp.exp(teacher_top - teacher_peak)
    return [
        peak,
        jnp.sum(total * jnp.exp(top - peak), axis=0, keepdims=True),
        teacher_peak,
        jnp.sum(teacher_total * scale, axis=0, keepdims=True),
        jnp.sum(cross * scale, axis=0, keepdims=True),
    ]


def add_terms(rows, hid_ref, acc, n, teacher, valid=None):
    size = rows.shape[1]
    hidden = hid_ref[n].reshape(rows.shape[0], -1)
    tokens = hidden.shape[1]
    student = lax.dot_general(rows, hidden, (((0,), (0,)), ((), ())), preferred_element_type=jnp.float32)
    teacher = teacher.astype(jnp.float32)
    if valid is not None:
        index = lax.broadcasted_iota(jnp.int32, student.shape, 0)
        keep = (index >= valid[0]) & (index < valid[1])
        student = jnp.where(keep, student, LOW)
        teacher = jnp.where(keep, teacher, LOW)
    student = student.reshape(size // 8, 8, tokens)
    teacher = teacher.reshape(size // 8, 8, tokens)
    top = jnp.maximum(acc[n, 0], jnp.max(student, axis=0))
    acc[n, 1] = acc[n, 1] * jnp.exp(acc[n, 0] - top) + jnp.sum(jnp.exp(student - top[None]), axis=0)
    acc[n, 0] = top
    teacher_top = jnp.maximum(acc[n, 2], jnp.max(teacher, axis=0))
    fade = jnp.exp(acc[n, 2] - teacher_top)
    weights = jnp.exp(teacher - teacher_top[None])
    acc[n, 3] = acc[n, 3] * fade + jnp.sum(weights, axis=0)
    acc[n, 4] = acc[n, 4] * fade + jnp.sum(weights * student, axis=0)
    acc[n, 2] = teacher_top


def kernel(
    rows, cols, depths, lay, emb_ref, teacher_ref, hidden_ref, sums_ref,
    table_ref, pack_ref, full_ref, half_ref, own_ref, other_ref, extra_ref, hid_ref, acc, stats_ref, held_ref,
    own_sem, first_send, first_recv, right_send, left_send, line_recv, teach_send, teach_recv, extra_send, extra_recv,
    hid_send, hid_recv, stats_send, stats_recv,
):
    r, c, d, q, j = place()
    steps = rows // GROUP
    count = depths * GROUP
    me = d * GROUP + j
    kept, whole, edge = lay.kept, lay.whole, lay.edge
    narrow = table_ref.shape[0]
    packed = narrow // 2
    end, server, inward = ends(rows, q)
    pj = lax.rem(j + 1, GROUP)
    pr = q * GROUP + pj
    slice_ = d * cols + c
    peers = []
    for dj in range(GROUP):
        for dc in range(cols):
            for dd in range(depths):
                if dj or dc or dd:
                    peers.append((q * GROUP + lax.rem(j + dj, GROUP), lax.rem(c + dc, cols), lax.rem(d + dd, depths), dj))
    group = [(r, c, d, 0)] + peers
    near = len(peers)
    same = [(a, b, e) for a, b, e, dj in peers if dj == 0]

    barrier = pltpu.get_barrier_semaphore()

    def greet(row, col, depth):
        pl.semaphore_signal(barrier, inc=1, device_id=(row, col, depth), device_id_type=MESH)

    @pl.when(q + 1 < steps)
    def _():
        greet(r + GROUP, c, d)

    @pl.when(q > 0)
    def _():
        greet(r - GROUP, c, d)

    for a, b, e, _ in peers:
        greet(a, b, e)

    def remote(source_ref, dst_ref, send_sem, recv_sem, device):
        return pltpu.make_async_remote_copy(
            src_ref=source_ref, dst_ref=dst_ref, send_sem=send_sem, recv_sem=recv_sem, device_id=device, device_id_type=MESH
        )

    load = pltpu.make_async_copy(emb_ref, table_ref, own_sem.at[0])
    load.start()
    load.wait()
    for target in range(count):
        part = table_ref[:, lay.stride * (target + 1) : lay.stride * (target + 1) + LANE // 2]
        pack_ref[target] = jnp.concatenate([part[:packed], part[packed:]], axis=1)

    def span(t):
        return pl.multiple_of(t * CHUNK, CHUNK), CHUNK, t, narrow

    ends_of = ((edge, lay.plain, whole, narrow), (lay.stride, LANE, whole + 1, packed))

    def piece(target, cut):
        first_lane, size, index, height = cut
        if height != narrow:
            return pack_ref.at[target]
        return table_ref.at[:, pl.ds(pl.multiple_of(lay.stride * target + first_lane, LANE), size)]

    def slot(depth, row, cut):
        first_lane, size, _, height = cut
        return full_ref.at[depth, row, :, pl.ds(first_lane, size)] if height == narrow else half_ref.at[depth, row]

    def block_at(block, cut):
        first_lane, size, _, height = cut
        row = pl.ds(pl.multiple_of(block * GROUP, GROUP), GROUP)
        return full_ref.at[:, row, :, pl.ds(first_lane, size)] if height == narrow else half_ref.at[:, row]

    own_piece = pltpu.make_async_copy(
        table_ref.at[:, pl.ds(pl.multiple_of(lay.stride * me, LANE), lay.stride)],
        full_ref.at[d, r], own_sem.at[1],
    )
    own_half = pltpu.make_async_copy(pack_ref.at[me], slot(d, r, ends_of[1]), own_sem.at[2])

    def kind(cut):
        return 0 if cut[3] == narrow else 1

    def first(cut, off):
        target = lax.rem(me + off, count)
        return remote(
            piece(target, cut), slot(d, r, cut), first_send.at[kind(cut)], first_recv.at[cut[2]],
            (q * GROUP + lax.rem(target, GROUP), c, target // GROUP),
        )

    def first_arrived(cut):
        row = pl.ds(0, count - 1)
        at = full_ref.at[0, row, :, pl.ds(cut[0], cut[1])] if cut[3] == narrow else half_ref.at[0, row]
        return remote(at, at, first_send.at[0], first_recv.at[cut[2]], (pr, c, d))

    def send_line(source_ref, dst_ref, block, cut, right):
        sems, place_ = (right_send, block) if right else (left_send, block - 1)
        return remote(
            source_ref, dst_ref, sems.at[block, kind(cut)], line_recv.at[place_, cut[2]],
            (r + GROUP if right else r - GROUP, c, d),
        )

    def along(block, cut, right):
        at = block_at(block, cut)
        return send_line(at, at, block, cut, right)

    def arrived(block, cut, right):
        at = block_at(block, cut)
        return remote(at, at, right_send.at[0, 0], line_recv.at[block if right else block - 1, cut[2]], (pr, c, d))

    def to_right(t):
        return (q + 1 < steps) & ((t < kept) | (q + 2 < steps))

    def to_left(t):
        return (q > 0) & ((t < kept) | (q > 1))

    def both(cut, source_ref, dst_ref):
        @pl.when(to_right(cut[2]))
        def _():
            send_line(source_ref, dst_ref, q, cut, True).start()

        @pl.when(to_left(cut[2]))
        def _():
            send_line(source_ref, dst_ref, q, cut, False).start()

    def give(n, sem, device, source_ref):
        return remote(source_ref, hid_ref.at[n, slice_], hid_send.at[sem], hid_recv.at[sem], device)

    cross = [give(1, 0, (pr, c, d), hidden_ref), None, give(3, 1, (pr, c, d), hid_ref.at[2, slice_])]
    far_hid = give(2, 2, (r + inward, c, d), hidden_ref)
    spread = [
        [give(n, 3 + n, device, hidden_ref if n == 0 else hid_ref.at[n, slice_]) for device in same] for n in range(2 * GROUP)
    ]

    def spread_all(n):
        at = hid_ref.at[n, pl.ds(0, len(same))]
        return remote(at, at, hid_send.at[3 + n], hid_recv.at[3 + n], (pr, c, d))

    pl.semaphore_wait(barrier, near + as_count(q + 1 < steps) + as_count(q > 0))

    @pl.when(end)
    def _():
        far_hid.start()

    def launch(cut):
        both(cut, piece(me, cut), slot(d, r, cut))
        for off in range(1, count):
            first(cut, off).start()

    loop(0, whole, lambda t: launch(span(t)))
    for cut in ends_of:
        launch(cut)

    cross[0].start()
    for copy in spread[0]:
        copy.start()

    has_head = ~((d > 0) & (j == 0))
    peer_head = ~((d > 0) & (pj == 0))
    has_tail = (d == depths - 1) & (j == GROUP - 1)
    peer_tail = (d == depths - 1) & (pj == GROUP - 1)
    shift = lay.shift * (depths - 1)

    def source(part, at, size):
        begin = jnp.clip(lay.stride * part - lay.shift * d + at, 0, lay.half - size)
        return teacher_ref.at[pl.ds(pl.multiple_of(begin, 16), size)]

    own_body = pltpu.make_async_copy(source(j, shift, lay.last - shift), own_ref.at[pl.ds(shift, lay.last - shift)], own_sem.at[3])
    own_head = pltpu.make_async_copy(source(j, 0, shift), own_ref.at[pl.ds(0, shift)], own_sem.at[4])
    own_tail = pltpu.make_async_copy(source(j, lay.last, shift), own_ref.at[pl.ds(lay.last, shift)], own_sem.at[5])
    own_hid = pltpu.make_async_copy(hidden_ref, hid_ref.at[0, slice_], own_sem.at[6])
    own_piece.start()
    own_half.start()
    own_hid.start()
    own_body.start()

    @pl.when(has_head)
    def _():
        own_head.start()

    @pl.when(has_tail)
    def _():
        own_tail.start()

    @pl.when(server)
    def _():
        far_hid.wait_recv()
        cross[2].start()
        for copy in spread[2]:
            copy.start()

    def start_line(cut):
        first_arrived(cut).wait_recv()
        for off in range(1, count):
            sender = lax.rem(me + count - off, count)
            at = slot(sender // GROUP, q * GROUP + lax.rem(sender, GROUP), cut)
            both(cut, at, at)

    loop(0, whole, lambda t: start_line(span(t)))
    for cut in ends_of:
        start_line(cut)

    body = lay.last - edge

    def teach_rows(index, at, size, sem=0):
        return remote(source(pj, at, size), other_ref.at[pl.ds(at, size)], teach_send.at[sem], teach_recv.at[index], (pr, c, d))

    def teach(t):
        return teach_rows(t, pl.multiple_of(t * CHUNK, CHUNK), CHUNK)

    teach_zero = teach_rows(0, shift, CHUNK - shift)
    teach_head = teach_rows(whole + 1, 0, shift, 1)
    teach_body = teach_rows(whole, edge, body)
    teach_tail = teach_rows(whole + 2, lay.last, shift, 2)

    def teach_kept():
        teach_zero.start()

        @pl.when(peer_head)
        def _():
            teach_head.start()

        loop(1, kept, lambda t: teach(t).start())

    def teach_rest():
        loop(kept, whole, lambda t: teach(t).start())
        teach_body.start()

        @pl.when(peer_tail)
        def _():
            teach_tail.start()

    @pl.when(end)
    def _():
        teach_rest()

    teach_kept()

    @pl.when(~end)
    def _():
        teach_rest()

    cross[0].wait_recv()
    for copy in spread[1]:
        copy.start()

    @pl.when(server)
    def _():
        cross[2].wait_recv()
        for copy in spread[3]:
            copy.start()

    def teach_end_arrived():
        teach_body.wait_recv()

        @pl.when(has_tail)
        def _():
            teach_tail.wait_recv()

    base = kept * CHUNK

    def extra_rows(n, index, at, size, sem=0):
        return remote(
            source(j, at, size) if n == 0 else other_ref.at[pl.ds(at, size)],
            extra_ref.at[n, pl.ds(at - base, size)], extra_send.at[sem], extra_recv.at[index], (r + inward, c, d),
        )

    def extra_arrived(index, at, size, sem=0):
        both_sets = extra_ref.at[:, pl.ds(at - base, size)]
        return remote(both_sets, both_sets, extra_send.at[sem], extra_recv.at[index], (pr, c, d))

    def extra_at(t):
        return t - kept, pl.multiple_of(t * CHUNK, CHUNK), CHUNK

    extra_body = (whole - kept, edge, body)
    extra_tail = (whole - kept + 1, lay.last, shift, 1)

    @pl.when(end)
    def _():
        def pass_on(t):
            teach(t).wait_recv()
            for n in range(GROUP):
                extra_rows(n, *extra_at(t)).start()

        loop(kept, whole, pass_on)
        teach_end_arrived()
        for n in range(GROUP):
            extra_rows(n, *extra_body).start()

        @pl.when(has_tail)
        def _():
            for n in range(GROUP):
                extra_rows(n, *extra_tail).start()

    def hop(k, cut):
        t = cut[2]
        wanted = (t < kept) | ~end

        @pl.when((q - k >= 0) & wanted)
        def _():
            arrived(q - k, cut, True).wait_recv()

            @pl.when(to_right(t))
            def _():
                along(q - k, cut, True).start()

        @pl.when((q + k < steps) & wanted)
        def _():
            arrived(q + k, cut, False).wait_recv()

            @pl.when(to_left(t))
            def _():
                along(q + k, cut, False).start()

    far = jnp.maximum(q, steps - 1 - q)

    def early(k):
        loop(0, whole, lambda t: hop(k, span(t)))
        for cut in ends_of:
            hop(k, cut)

    loop(1, far, early)

    for n in range(2 * GROUP):
        for k in range(5):
            acc[n, k] = jnp.full(acc.shape[2:], LOW if k in (0, 2) else 0.0, jnp.float32)

    def features(t):
        return full_ref[:, :, :, pl.ds(pl.multiple_of(t * CHUNK, CHUNK), CHUNK)].reshape(-1, CHUNK)

    def end_features():
        tile = full_ref[:, :, :, edge:].reshape(-1, lay.plain)
        half = half_ref[...]
        half = jnp.concatenate([half[..., : LANE // 2], half[..., LANE // 2 :]], axis=2).reshape(-1, LANE // 2)
        return jnp.concatenate([tile, half], axis=1)

    def main(rows_, at, valid=None):
        for n, ref in enumerate((own_ref, other_ref)):
            add_terms(rows_, hid_ref, acc, n, ref[at, :], valid)

    def more(rows_, at, valid=None):
        for n in range(GROUP):
            add_terms(rows_, hid_ref, acc, GROUP + n, extra_ref[n, at, :], valid)

    def rows_at(t):
        return pl.ds(pl.multiple_of(t * CHUNK, CHUNK), CHUNK)

    hop(far, span(0))
    own_body.wait()

    @pl.when(has_head)
    def _():
        own_head.wait()

    @pl.when(has_tail)
    def _():
        own_tail.wait()

    own_hid.wait()
    own_piece.wait()
    own_half.wait()
    for n in range(2):
        spread_all(n).wait_recv()
    teach_zero.wait_recv()

    @pl.when(has_head)
    def _():
        teach_head.wait_recv()

    main(features(0), rows_at(0), (jnp.where(has_head, 0, shift), CHUNK))

    def kept_chunk(t):
        hop(far, span(t))
        teach(t).wait_recv()
        main(features(t), rows_at(t))

    loop(1, kept, kept_chunk)

    @pl.when(server)
    def _():
        for n in range(2, 4):
            spread_all(n).wait_recv()

    @pl.when(~end)
    def _():
        def rest_chunk(t):
            hop(far, span(t))

            @pl.when(server)
            def _():
                extra_arrived(*extra_at(t)).wait_recv()
                more(features(t), rows_at(t - kept))

            teach(t).wait_recv()
            main(features(t), rows_at(t))

        loop(kept, whole, rest_chunk)
        for cut in ends_of:
            hop(far, cut)

    def close(n):
        values = merge([acc[n, k] for k in range(5)])
        stats_ref[n] = jnp.concatenate(values + [values[0]] * 3, axis=0)

    def tell(n, sem, device, source_set):
        return remote(stats_ref.at[source_set], held_ref.at[n], stats_send.at[sem], stats_recv.at[sem], device)

    def told(sem, begin, size):
        at = held_ref.at[pl.ds(begin, size)]
        return remote(at, at, stats_send.at[sem], stats_recv.at[sem], (pr, c, d))

    limit = (0, jnp.where(j == 0, lay.stride, lay.last + lay.shift * d) - edge)

    @pl.when(server)
    def _():
        extra_arrived(*extra_body).wait_recv()

        @pl.when(has_tail)
        def _():
            extra_arrived(*extra_tail).wait_recv()

        more(end_features(), pl.ds(edge - base, lay.rest), limit)
        for n in range(GROUP, 2 * GROUP):
            close(n)
        for n, (a, b, e, dj) in enumerate(group):
            tell(near + n, 1, (a - inward, b, e), GROUP + dj).start()

    @pl.when(~end)
    def _():
        teach_end_arrived()
        main(end_features(), pl.ds(edge, lay.rest), limit)

    for n in range(GROUP):
        close(n)
    for n, (a, b, e, dj) in enumerate(peers):
        tell(n, 0, (a, b, e), dj).start()

    @pl.when(~end)
    def _():
        for n in range(len(group)):
            for k in range(5):
                held_ref[near + n, k] = jnp.full(held_ref.shape[2:], LOW if k in (0, 2) else 0.0, jnp.float32)

    def settle(block):
        def sent(right, size):
            at = block_at(block, (0, size, 0, narrow))
            remote(at, at, (right_send if right else left_send).at[block, 0], line_recv.at[0, 0], (pr, c, d)).wait_send()

        def sent_half(right):
            at = block_at(block, ends_of[1])
            remote(at, at, (right_send if right else left_send).at[block, 1], line_recv.at[0, 0], (pr, c, d)).wait_send()

        @pl.when((block <= q) & (q + 2 < steps))
        def _():
            sent(True, lay.stride)
            sent_half(True)

        @pl.when((block <= q) & (q + 2 == steps))
        def _():
            sent(True, base)

        @pl.when((block >= q) & (q > 1))
        def _():
            sent(False, lay.stride)
            sent_half(False)

        @pl.when((block >= q) & (q == 1))
        def _():
            sent(False, base)

    loop(0, steps, settle)
    sent_pieces = full_ref.at[0, pl.ds(0, count - 1)]
    remote(sent_pieces, sent_pieces, first_send.at[0], first_recv.at[0], (pr, c, d)).wait_send()
    sent_halves = half_ref.at[0, pl.ds(0, count - 1)]
    remote(sent_halves, sent_halves, first_send.at[1], first_recv.at[0], (pr, c, d)).wait_send()
    cross[0].wait_send()
    for n in range(2):
        spread_all(n).wait_send()
    taught = other_ref.at[pl.ds(shift, lay.last - shift)]
    remote(taught, taught, teach_send.at[0], teach_recv.at[0], (pr, c, d)).wait_send()

    @pl.when(peer_head)
    def _():
        teach_head.wait_send()

    @pl.when(peer_tail)
    def _():
        teach_tail.wait_send()

    @pl.when(end)
    def _():
        far_hid.wait_send()
        extra_arrived(0, base, lay.last - base).wait_send()

        @pl.when(has_tail)
        def _():
            extra_arrived(*extra_tail).wait_send()

    @pl.when(server)
    def _():
        cross[2].wait_send()
        for n in range(2, 4):
            spread_all(n).wait_send()
        told(1, near, len(group)).wait_send()

    told(0, 0, near).wait()

    @pl.when(end)
    def _():
        told(1, near, len(group)).wait_recv()

    blocks = [stats_ref[0]] + [held_ref[n] for n in range(near + len(group))]
    parts = [jnp.concatenate([block[k : k + 1] for block in blocks], axis=0) for k in range(5)]
    peak, total, _, teacher_total, cross_sum = merge(parts)
    sums_ref[...] = jnp.concatenate([peak, total, teacher_total, cross_sum] + [peak] * 4, axis=0)


def on_device(rows, cols, depths, student_hidden, embedding, teacher_logits):
    vocab, narrow = embedding.shape
    lay = Layout(vocab, depths)
    hidden = student_hidden.T
    features, tokens = hidden.shape
    steps = rows // GROUP
    slots = 2 * GROUP * cols * depths - 1
    whole, height = lay.whole, lay.edge + lay.rest
    dma = pltpu.SemaphoreType.DMA
    any_space = pl.BlockSpec(memory_space=pl.ANY)
    dtype = embedding.dtype
    sums = pl.pallas_call(
        functools.partial(kernel, rows, cols, depths, lay),
        out_shape=jax.ShapeDtypeStruct((8, tokens), jnp.float32),
        in_specs=[any_space] * 3,
        out_specs=pl.BlockSpec(memory_space=pltpu.VMEM),
        scratch_shapes=[
            pltpu.VMEM((narrow, vocab), dtype),
            pltpu.VMEM((depths * GROUP, narrow // 2, LANE), dtype),
            pltpu.VMEM((depths, rows, narrow, lay.stride), dtype),
            pltpu.VMEM((depths, rows, narrow // 2, LANE), dtype),
            pltpu.VMEM((height, tokens), teacher_logits.dtype),
            pltpu.VMEM((height, tokens), teacher_logits.dtype),
            pltpu.VMEM((GROUP, height - lay.kept * CHUNK, tokens), teacher_logits.dtype),
            pltpu.VMEM((2 * GROUP, depths * cols, features, tokens), hidden.dtype),
            pltpu.VMEM((2 * GROUP, 5, 8, tokens), jnp.float32),
            pltpu.VMEM((2 * GROUP, 8, tokens), jnp.float32),
            pltpu.VMEM((slots, 8, tokens), jnp.float32),
            dma((7,)), dma((2,)), dma((whole + 2,)), dma((steps, 2)), dma((steps, 2)), dma((steps - 1, whole + 2)),
            dma((3,)), dma((whole + 3,)), dma((2,)), dma((whole - lay.kept + 2,)),
            dma((3 + 2 * GROUP,)), dma((3 + 2 * GROUP,)), dma((2,)), dma((2,)),
        ],
        compiler_params=pltpu.CompilerParams(collective_id=0, has_side_effects=True, vmem_limit_bytes=60 * 2**20),
        name="distill",
    )(embedding.T, teacher_logits.T, hidden)
    norm_log = jnp.log(sums[1])
    return sums[0] + norm_log - sums[3] / sums[2], -norm_log


def solution(mesh):
    sizes = [mesh.shape[name] for name in ("row", "col", "depth")]
    in_specs = (P("row", ("depth", "col")), P("col", ("depth", "row")), P("row", ("col", "depth")))
    out_specs = (P("row"), P("row"))
    return jax.shard_map(
        functools.partial(on_device, *sizes), mesh=mesh, in_specs=in_specs, out_specs=out_specs, check_vma=False
    )
```

```python
import functools

import jax
import jax.numpy as jnp
from jax import lax
from jax.experimental import pallas as pl
from jax.experimental.pallas import tpu as pltpu
from jax.sharding import PartitionSpec as P

MESH = pl.DeviceIdType.MESH
GROUP = 2
LANE = 128
CHUNK = 384
KEPT = 0.67
LOW = -1e30


class Layout:
    def __init__(self, vocab, depths):
        self.half = vocab // depths
        self.stride = vocab // LANE // (depths * GROUP) * LANE
        self.shift = self.half - GROUP * self.stride
        self.last = self.half - (GROUP - 1) * self.stride
        self.edge = (self.stride - LANE) // CHUNK * CHUNK
        self.whole = self.edge // CHUNK
        self.plain = self.stride - self.edge
        self.rest = self.plain + LANE // 2
        self.kept = round(self.stride / CHUNK * KEPT)
        assert depths == 2 and 0 <= self.shift < CHUNK and self.shift % 16 == 0
        assert self.last + self.shift <= self.stride + LANE // 2 and self.plain % LANE == 0
        assert vocab <= self.stride * depths * GROUP + LANE // 2


def place():
    r, c, d = lax.axis_index("row"), lax.axis_index("col"), lax.axis_index("depth")
    return r, c, d, r // GROUP, lax.rem(r, GROUP)


def ends(rows, q):
    steps = rows // GROUP
    low, high = q == 0, q == steps - 1
    return low | high, (q == 1) | (q == steps - 2), jnp.where(q * 2 < steps, GROUP, -GROUP)


def as_count(flag):
    return flag.astype(jnp.int32)


def loop(begin, stop, body):
    def step(i, _):
        body(i)
        return 0

    lax.fori_loop(begin, stop, step, 0)


def gather_terms(parts):
    top, total, teacher_top, teacher_total, cross = parts
    peak = jnp.max(top, axis=0, keepdims=True)
    teacher_peak = jnp.max(teacher_top, axis=0, keepdims=True)
    scale = jnp.exp(teacher_top - teacher_peak)
    weight = jnp.sum(teacher_total * scale, axis=0, keepdims=True)
    return [
        peak,
        jnp.sum(total * jnp.exp(top - peak), axis=0, keepdims=True),
        teacher_peak + jnp.log(weight),
        jnp.sum(cross * scale, axis=0, keepdims=True) / weight,
    ]


def fold(values):
    whole = jnp.concatenate(values, axis=0)
    half = whole.shape[1] // 2
    return jnp.concatenate([whole[:, :half], whole[:, half:]], axis=0)


def product(rows, hidden):
    return lax.dot_general(rows, hidden, (((0,), (0,)), ((), ())), preferred_element_type=jnp.float32)


def add_terms(student, acc, at, teacher, valid=None):
    size = student.shape[0]
    teacher = teacher.astype(jnp.float32)
    if valid is not None:
        index = lax.broadcasted_iota(jnp.int32, student.shape, 0)
        keep = (index >= valid[0]) & (index < valid[1])
        student = jnp.where(keep, student, LOW)
        teacher = jnp.where(keep, teacher, LOW)
    student = student.reshape(size // 8, 8, -1)
    teacher = teacher.reshape(size // 8, 8, -1)
    old, teacher_old = acc[0, :, at], acc[2, :, at]
    top = jnp.maximum(old, jnp.max(student, axis=0))
    acc[1, :, at] = acc[1, :, at] * jnp.exp(old - top) + jnp.sum(jnp.exp(student - top[None]), axis=0)
    acc[0, :, at] = top
    teacher_top = jnp.maximum(teacher_old, jnp.max(teacher, axis=0))
    fade = jnp.exp(teacher_old - teacher_top)
    weights = jnp.exp(teacher - teacher_top[None])
    acc[3, :, at] = acc[3, :, at] * fade + jnp.sum(weights, axis=0)
    acc[4, :, at] = acc[4, :, at] * fade + jnp.sum(weights * student, axis=0)
    acc[2, :, at] = teacher_top


def kernel(
    rows, cols, depths, lay, emb_ref, teacher_ref, hidden_ref, sums_ref,
    table_ref, pack_ref, full_ref, half_ref, own_ref, other_ref, extra_ref, hid_ref, acc, ahead_ref, stats_ref, held_ref,
    own_sem, first_send, first_recv, right_send, left_send, line_recv, teach_send, teach_recv, extra_send, extra_recv,
    hid_send, hid_recv, stats_send, stats_recv,
):
    r, c, d, q, j = place()
    steps = rows // GROUP
    count = depths * GROUP
    me = d * GROUP + j
    kept, whole, edge = lay.kept, lay.whole, lay.edge
    narrow = table_ref.shape[0]
    packed = narrow // 2
    tokens = hidden_ref.shape[1]
    end, server, inward = ends(rows, q)
    pj = lax.rem(j + 1, GROUP)
    pr = q * GROUP + pj
    slice_ = d * cols + c
    peers = []
    for dj in range(GROUP):
        for dc in range(cols):
            for dd in range(depths):
                if dj or dc or dd:
                    peers.append((q * GROUP + lax.rem(j + dj, GROUP), lax.rem(c + dc, cols), lax.rem(d + dd, depths), dj))
    group = [(r, c, d, 0)] + peers
    near = len(peers)
    same = [(a, b, e) for a, b, e, dj in peers if dj == 0]

    barrier = pltpu.get_barrier_semaphore()

    def greet(row, col, depth):
        pl.semaphore_signal(barrier, inc=1, device_id=(row, col, depth), device_id_type=MESH)

    @pl.when(q + 1 < steps)
    def _():
        greet(r + GROUP, c, d)

    @pl.when(q > 0)
    def _():
        greet(r - GROUP, c, d)

    for a, b, e, _ in peers:
        greet(a, b, e)

    def remote(source_ref, dst_ref, send_sem, recv_sem, device):
        return pltpu.make_async_remote_copy(
            src_ref=source_ref, dst_ref=dst_ref, send_sem=send_sem, recv_sem=recv_sem, device_id=device, device_id_type=MESH
        )

    load = pltpu.make_async_copy(emb_ref, table_ref, own_sem.at[0])
    load.start()
    load.wait()
    for target in range(count):
        part = table_ref[:, lay.stride * (target + 1) : lay.stride * (target + 1) + LANE // 2]
        pack_ref[target] = jnp.concatenate([part[:packed], part[packed:]], axis=1)

    def span(t):
        return pl.multiple_of(t * CHUNK, CHUNK), CHUNK, t, narrow

    ends_of = ((edge, lay.plain, whole, narrow), (lay.stride, LANE, whole + 1, packed))

    def piece(target, cut):
        first_lane, size, index, height = cut
        if height != narrow:
            return pack_ref.at[target]
        return table_ref.at[:, pl.ds(pl.multiple_of(lay.stride * target + first_lane, LANE), size)]

    def slot(depth, row, cut):
        first_lane, size, _, height = cut
        return full_ref.at[depth, row, :, pl.ds(first_lane, size)] if height == narrow else half_ref.at[depth, row]

    def block_at(block, cut):
        first_lane, size, _, height = cut
        row = pl.ds(pl.multiple_of(block * GROUP, GROUP), GROUP)
        return full_ref.at[:, row, :, pl.ds(first_lane, size)] if height == narrow else half_ref.at[:, row]

    own_piece = pltpu.make_async_copy(
        table_ref.at[:, pl.ds(pl.multiple_of(lay.stride * me, LANE), lay.stride)],
        full_ref.at[d, r], own_sem.at[1],
    )
    own_half = pltpu.make_async_copy(pack_ref.at[me], slot(d, r, ends_of[1]), own_sem.at[2])

    def kind(cut):
        return 0 if cut[3] == narrow else 1

    def first(cut, off):
        target = lax.rem(me + off, count)
        return remote(
            piece(target, cut), slot(d, r, cut), first_send.at[kind(cut)], first_recv.at[cut[2]],
            (q * GROUP + lax.rem(target, GROUP), c, target // GROUP),
        )

    def first_arrived(cut):
        row = pl.ds(0, count - 1)
        at = full_ref.at[0, row, :, pl.ds(cut[0], cut[1])] if cut[3] == narrow else half_ref.at[0, row]
        return remote(at, at, first_send.at[0], first_recv.at[cut[2]], (pr, c, d))

    def send_line(source_ref, dst_ref, block, cut, right):
        sems, place_ = (right_send, block) if right else (left_send, block - 1)
        return remote(
            source_ref, dst_ref, sems.at[block, kind(cut)], line_recv.at[place_, cut[2]],
            (r + GROUP if right else r - GROUP, c, d),
        )

    def along(block, cut, right):
        at = block_at(block, cut)
        return send_line(at, at, block, cut, right)

    def arrived(block, cut, right):
        at = block_at(block, cut)
        return remote(at, at, right_send.at[0, 0], line_recv.at[block if right else block - 1, cut[2]], (pr, c, d))

    def to_right(t):
        return (q + 1 < steps) & ((t < kept) | (q + 2 < steps))

    def to_left(t):
        return (q > 0) & ((t < kept) | (q > 1))

    def both(cut, source_ref, dst_ref):
        @pl.when(to_right(cut[2]))
        def _():
            send_line(source_ref, dst_ref, q, cut, True).start()

        @pl.when(to_left(cut[2]))
        def _():
            send_line(source_ref, dst_ref, q, cut, False).start()

    def hidden_at(n, where=None):
        return hid_ref.at[slice_ if where is None else where, :, pl.ds(n * tokens, tokens)]

    def give(n, sem, device, source_ref):
        return remote(source_ref, hidden_at(n), hid_send.at[sem], hid_recv.at[sem], device)

    cross = [give(1, 0, (pr, c, d), hidden_ref), None, give(3, 1, (pr, c, d), hidden_at(2))]
    far_hid = give(2, 2, (r + inward, c, d), hidden_ref)
    spread = [
        [give(n, 3 + n, device, hidden_ref if n == 0 else hidden_at(n)) for device in same] for n in range(2 * GROUP)
    ]

    def spread_all(n):
        at = hidden_at(n, pl.ds(0, len(same)))
        return remote(at, at, hid_send.at[3 + n], hid_recv.at[3 + n], (pr, c, d))

    pl.semaphore_wait(barrier, near + as_count(q + 1 < steps) + as_count(q > 0))

    @pl.when(end)
    def _():
        far_hid.start()

    def launch(cut):
        both(cut, piece(me, cut), slot(d, r, cut))
        for off in range(1, count):
            first(cut, off).start()

    loop(0, whole, lambda t: launch(span(t)))
    for cut in ends_of:
        launch(cut)

    cross[0].start()
    for copy in spread[0]:
        copy.start()

    has_head = ~((d > 0) & (j == 0))
    peer_head = ~((d > 0) & (pj == 0))
    has_tail = (d == depths - 1) & (j == GROUP - 1)
    peer_tail = (d == depths - 1) & (pj == GROUP - 1)
    shift = lay.shift * (depths - 1)

    def source(part, at, size):
        begin = jnp.clip(lay.stride * part - lay.shift * d + at, 0, lay.half - size)
        return teacher_ref.at[pl.ds(pl.multiple_of(begin, 16), size)]

    own_body = pltpu.make_async_copy(source(j, shift, lay.last - shift), own_ref.at[pl.ds(shift, lay.last - shift)], own_sem.at[3])
    own_head = pltpu.make_async_copy(source(j, 0, shift), own_ref.at[pl.ds(0, shift)], own_sem.at[4])
    own_tail = pltpu.make_async_copy(source(j, lay.last, shift), own_ref.at[pl.ds(lay.last, shift)], own_sem.at[5])
    own_hid = pltpu.make_async_copy(hidden_ref, hidden_at(0), own_sem.at[6])
    own_piece.start()
    own_half.start()
    own_hid.start()
    own_body.start()

    @pl.when(has_head)
    def _():
        own_head.start()

    @pl.when(has_tail)
    def _():
        own_tail.start()

    @pl.when(server)
    def _():
        far_hid.wait_recv()
        cross[2].start()
        for copy in spread[2]:
            copy.start()

    def start_line(cut):
        first_arrived(cut).wait_recv()
        for off in range(1, count):
            sender = lax.rem(me + count - off, count)
            at = slot(sender // GROUP, q * GROUP + lax.rem(sender, GROUP), cut)
            both(cut, at, at)

    loop(0, whole, lambda t: start_line(span(t)))
    for cut in ends_of:
        start_line(cut)

    body = lay.last - edge

    def teach_rows(index, at, size, sem=0):
        return remote(source(pj, at, size), other_ref.at[pl.ds(at, size)], teach_send.at[sem], teach_recv.at[index], (pr, c, d))

    def teach(t):
        return teach_rows(t, pl.multiple_of(t * CHUNK, CHUNK), CHUNK)

    teach_zero = teach_rows(0, shift, CHUNK - shift)
    teach_head = teach_rows(whole + 1, 0, shift, 1)
    teach_body = teach_rows(whole, edge, body)
    teach_tail = teach_rows(whole + 2, lay.last, shift, 2)

    def teach_kept():
        teach_zero.start()

        @pl.when(peer_head)
        def _():
            teach_head.start()

        loop(1, kept, lambda t: teach(t).start())

    def teach_rest():
        loop(kept, whole, lambda t: teach(t).start())
        teach_body.start()

        @pl.when(peer_tail)
        def _():
            teach_tail.start()

    @pl.when(end)
    def _():
        teach_rest()

    teach_kept()

    @pl.when(~end)
    def _():
        teach_rest()

    cross[0].wait_recv()
    for copy in spread[1]:
        copy.start()

    @pl.when(server)
    def _():
        cross[2].wait_recv()
        for copy in spread[3]:
            copy.start()

    def teach_end_arrived():
        teach_body.wait_recv()

        @pl.when(has_tail)
        def _():
            teach_tail.wait_recv()

    base = kept * CHUNK

    def extra_rows(n, index, at, size, sem=0):
        return remote(
            source(j, at, size) if n == 0 else other_ref.at[pl.ds(at, size)],
            extra_ref.at[n, pl.ds(at - base, size)], extra_send.at[sem], extra_recv.at[index], (r + inward, c, d),
        )

    def extra_arrived(index, at, size, sem=0):
        both_sets = extra_ref.at[:, pl.ds(at - base, size)]
        return remote(both_sets, both_sets, extra_send.at[sem], extra_recv.at[index], (pr, c, d))

    def extra_at(t):
        return t - kept, pl.multiple_of(t * CHUNK, CHUNK), CHUNK

    extra_body = (whole - kept, edge, body)
    extra_tail = (whole - kept + 1, lay.last, shift, 1)

    @pl.when(end)
    def _():
        def pass_on(t):
            teach(t).wait_recv()
            for n in range(GROUP):
                extra_rows(n, *extra_at(t)).start()

        loop(kept, whole, pass_on)
        teach_end_arrived()
        for n in range(GROUP):
            extra_rows(n, *extra_body).start()

        @pl.when(has_tail)
        def _():
            for n in range(GROUP):
                extra_rows(n, *extra_tail).start()

    def hop(k, cut):
        t = cut[2]
        wanted = (t < kept) | ~end

        @pl.when((q - k >= 0) & wanted)
        def _():
            arrived(q - k, cut, True).wait_recv()

            @pl.when(to_right(t))
            def _():
                along(q - k, cut, True).start()

        @pl.when((q + k < steps) & wanted)
        def _():
            arrived(q + k, cut, False).wait_recv()

            @pl.when(to_left(t))
            def _():
                along(q + k, cut, False).start()

    far = jnp.maximum(q, steps - 1 - q)

    def early(k):
        loop(0, whole, lambda t: hop(k, span(t)))
        for cut in ends_of:
            hop(k, cut)

    loop(1, far, early)

    for k in range(5):
        acc[k] = jnp.full(acc.shape[1:], LOW if k in (0, 2) else 0.0, jnp.float32)

    def features(t):
        return full_ref[:, :, :, pl.ds(pl.multiple_of(t * CHUNK, CHUNK), CHUNK)].reshape(-1, CHUNK)

    def token_lanes(sets):
        return pl.ds(sets[0] * tokens, len(sets) * tokens)

    def hidden_of(sets):
        return hid_ref[:, :, token_lanes(sets)].reshape(-1, len(sets) * tokens)

    def unpacked(half):
        half = jnp.concatenate([half[..., : LANE // 2], half[..., LANE // 2 :]], axis=2)
        return half.reshape(-1, LANE // 2)

    def tile_features(block=None):
        at = pl.ds(0, rows) if block is None else pl.ds(block * GROUP, GROUP)
        return full_ref[:, at, :, edge:].reshape(-1, lay.plain)

    def half_features(block=None):
        return unpacked(half_ref[:, pl.ds(0, rows) if block is None else pl.ds(block * GROUP, GROUP)])

    def hidden_block(block, sets):
        begin = block * (GROUP * narrow)
        at = pl.ds(pl.multiple_of(lax.rem(begin, hid_ref.shape[1]), 16), GROUP * narrow)
        parts = [hid_ref[depth * cols + begin // hid_ref.shape[1], at, token_lanes(sets)] for depth in range(depths)]
        return jnp.concatenate(parts, axis=0)

    def main(rows_, at, valid=None):
        for n, ref in enumerate((own_ref, other_ref)):
            add_terms(product(rows_, hidden_of((n,))), acc, token_lanes((n,)), ref[at, :], valid)

    def more(rows_, at):
        for n in range(GROUP):
            add_terms(product(rows_, hidden_of((GROUP + n,))), acc, token_lanes((GROUP + n,)), extra_ref[n, at, :])

    def teacher_of(sets, begin, size):
        at = pl.ds(begin, size)
        own = [own_ref[at, :], other_ref[at, :]]
        taken = [extra_ref[n, pl.ds(begin - base, size), :] for n in range(GROUP)] if len(sets) > GROUP else []
        return jnp.concatenate(own + taken, axis=1)

    ahead = steps <= 4 and narrow % 32 == 16 and hid_ref.shape[1] % (GROUP * narrow) == 0
    last_block = jnp.where(q * 2 < steps, steps - 1, 0)

    def prepare(sets):
        if not ahead:
            return
        tile = half = None
        for n in range(1, steps):
            block = lax.rem(last_block + n, steps)
            hidden = hidden_block(block, sets)
            tile_part, half_part = product(tile_features(block), hidden), product(half_features(block), hidden)
            tile, half = (tile_part, half_part) if tile is None else (tile + tile_part, half + half_part)
        ahead_ref[pl.ds(0, lay.plain), token_lanes(sets)] = tile
        ahead_ref[pl.ds(lay.plain, LANE // 2), token_lanes(sets)] = half

    def end_student(sets, take, begin, size):
        if not ahead:
            return product(take(), hidden_of(sets))
        return ahead_ref[pl.ds(begin, size), token_lanes(sets)] + product(take(last_block), hidden_block(last_block, sets))

    def rows_at(t):
        return pl.ds(pl.multiple_of(t * CHUNK, CHUNK), CHUNK)

    hop(far, span(0))
    own_body.wait()

    @pl.when(has_head)
    def _():
        own_head.wait()

    @pl.when(has_tail)
    def _():
        own_tail.wait()

    own_hid.wait()
    own_piece.wait()
    own_half.wait()
    for n in range(2):
        spread_all(n).wait_recv()
    teach_zero.wait_recv()

    @pl.when(has_head)
    def _():
        teach_head.wait_recv()

    main(features(0), rows_at(0), (jnp.where(has_head, 0, shift), CHUNK))

    def kept_chunk(t):
        hop(far, span(t))
        teach(t).wait_recv()
        main(features(t), rows_at(t))

    loop(1, kept, kept_chunk)

    @pl.when(server)
    def _():
        for n in range(2, 4):
            spread_all(n).wait_recv()

    @pl.when(~end)
    def _():
        def rest_chunk(t):
            hop(far, span(t))

            teach(t).wait_recv()
            main(features(t), rows_at(t))

            @pl.when(server)
            def _():
                extra_arrived(*extra_at(t)).wait_recv()
                more(features(t), rows_at(t - kept))

        loop(kept, whole - 1, rest_chunk)

        @pl.when(server)
        def _():
            prepare(tuple(range(2 * GROUP)))

        @pl.when(~server)
        def _():
            prepare(tuple(range(GROUP)))

        rest_chunk(whole - 1)

    def close(sets):
        at = pl.ds(sets[0] * tokens, len(sets) * tokens)
        values = gather_terms([acc[k, :, at] for k in range(5)])
        for n in range(len(sets)):
            stats_ref[sets[n]] = fold([value[:, n * tokens : (n + 1) * tokens] for value in values])

    def tell(n, sem, device, source_set):
        return remote(stats_ref.at[source_set], held_ref.at[n], stats_send.at[sem], stats_recv.at[sem], device)

    def told(sem, begin, size):
        at = held_ref.at[pl.ds(begin, size)]
        return remote(at, at, stats_send.at[sem], stats_recv.at[sem], (pr, c, d))

    limit = (0, lay.last + lay.shift * d - lay.stride)
    half_used = j == GROUP - 1

    own_sets, all_sets = tuple(range(GROUP)), tuple(range(2 * GROUP))

    def tell_near():
        for n, (a, b, e, dj) in reversed(list(enumerate(peers))):
            tell(n, 0, (a, b, e), dj).start()

    def finish(sets):
        at = token_lanes(sets)
        student = end_student(sets, tile_features, 0, lay.plain)
        add_terms(student, acc, at, teacher_of(sets, edge, lay.plain))
        hop(far, ends_of[1])

        @pl.when(half_used)
        def _():
            student = end_student(sets, half_features, lay.plain, LANE // 2)
            add_terms(student, acc, at, teacher_of(sets, lay.stride, LANE // 2), limit)

        close(sets)

    @pl.when(~end)
    def _():
        hop(far, ends_of[0])
        teach_end_arrived()

    @pl.when(server)
    def _():
        extra_arrived(*extra_body).wait_recv()

        @pl.when(has_tail)
        def _():
            extra_arrived(*extra_tail).wait_recv()

        finish(all_sets)
        for n, (a, b, e, dj) in reversed(list(enumerate(group))):
            tell(near + n, 1, (a - inward, b, e), GROUP + dj).start()

    @pl.when(~end & ~server)
    def _():
        finish(own_sets)

    @pl.when(end)
    def _():
        close(own_sets)

    tell_near()

    @pl.when(~end)
    def _():
        kinds = lax.broadcasted_iota(jnp.int32, held_ref.shape[1:], 0) % 2
        for n in range(len(group)):
            held_ref[near + n] = jnp.where(kinds == 0, LOW, 0.0)

    def settle(block):
        def sent(right, size):
            at = block_at(block, (0, size, 0, narrow))
            remote(at, at, (right_send if right else left_send).at[block, 0], line_recv.at[0, 0], (pr, c, d)).wait_send()

        def sent_half(right):
            at = block_at(block, ends_of[1])
            remote(at, at, (right_send if right else left_send).at[block, 1], line_recv.at[0, 0], (pr, c, d)).wait_send()

        @pl.when((block <= q) & (q + 2 < steps))
        def _():
            sent(True, lay.stride)
            sent_half(True)

        @pl.when((block <= q) & (q + 2 == steps))
        def _():
            sent(True, base)

        @pl.when((block >= q) & (q > 1))
        def _():
            sent(False, lay.stride)
            sent_half(False)

        @pl.when((block >= q) & (q == 1))
        def _():
            sent(False, base)

    loop(0, steps, settle)
    sent_pieces = full_ref.at[0, pl.ds(0, count - 1)]
    remote(sent_pieces, sent_pieces, first_send.at[0], first_recv.at[0], (pr, c, d)).wait_send()
    sent_halves = half_ref.at[0, pl.ds(0, count - 1)]
    remote(sent_halves, sent_halves, first_send.at[1], first_recv.at[0], (pr, c, d)).wait_send()
    cross[0].wait_send()
    for n in range(2):
        spread_all(n).wait_send()
    taught = other_ref.at[pl.ds(shift, lay.last - shift)]
    remote(taught, taught, teach_send.at[0], teach_recv.at[0], (pr, c, d)).wait_send()

    @pl.when(peer_head)
    def _():
        teach_head.wait_send()

    @pl.when(peer_tail)
    def _():
        teach_tail.wait_send()

    @pl.when(end)
    def _():
        far_hid.wait_send()
        extra_arrived(0, base, lay.last - base).wait_send()

        @pl.when(has_tail)
        def _():
            extra_arrived(*extra_tail).wait_send()

    @pl.when(server)
    def _():
        cross[2].wait_send()
        for n in range(2, 4):
            spread_all(n).wait_send()
        told(1, near, len(group)).wait_send()

    told(0, 0, near).wait()

    @pl.when(end)
    def _():
        told(1, near, len(group)).wait_recv()

    blocks = [stats_ref[0]] + [held_ref[n] for n in range(near + len(group))]
    top = functools.reduce(jnp.maximum, blocks)
    scales = [jnp.exp(block - top) for block in blocks]
    weight = functools.reduce(jnp.add, scales)
    scaled = functools.reduce(jnp.add, [block * pltpu.roll(scale, 1, 0) for block, scale in zip(blocks, scales)])
    row_kind = lax.broadcasted_iota(jnp.int32, top.shape, 0) % 4
    sums_ref[...] = jnp.where(row_kind == 0, top, jnp.where(row_kind == 2, weight, scaled))


def on_device(rows, cols, depths, student_hidden, embedding, teacher_logits):
    vocab, narrow = embedding.shape
    lay = Layout(vocab, depths)
    hidden = student_hidden.T
    features, tokens = hidden.shape
    steps = rows // GROUP
    slots = 2 * GROUP * cols * depths - 1
    whole, height = lay.whole, lay.edge + lay.rest
    dma = pltpu.SemaphoreType.DMA
    any_space = pl.BlockSpec(memory_space=pl.ANY)
    dtype = embedding.dtype
    sums = pl.pallas_call(
        functools.partial(kernel, rows, cols, depths, lay),
        out_shape=jax.ShapeDtypeStruct((8, tokens // 2), jnp.float32),
        in_specs=[any_space] * 3,
        out_specs=pl.BlockSpec(memory_space=pltpu.VMEM),
        scratch_shapes=[
            pltpu.VMEM((narrow, vocab), dtype),
            pltpu.VMEM((depths * GROUP, narrow // 2, LANE), dtype),
            pltpu.VMEM((depths, rows, narrow, lay.stride), dtype),
            pltpu.VMEM((depths, rows, narrow // 2, LANE), dtype),
            pltpu.VMEM((height, tokens), teacher_logits.dtype),
            pltpu.VMEM((height, tokens), teacher_logits.dtype),
            pltpu.VMEM((GROUP, height - lay.kept * CHUNK, tokens), teacher_logits.dtype),
            pltpu.VMEM((depths * cols, features, 2 * GROUP * tokens), hidden.dtype),
            pltpu.VMEM((5, 8, 2 * GROUP * tokens), jnp.float32),
            pltpu.VMEM((lay.rest, 2 * GROUP * tokens), jnp.float32),
            pltpu.VMEM((2 * GROUP, 8, tokens // 2), jnp.float32),
            pltpu.VMEM((slots, 8, tokens // 2), jnp.float32),
            dma((7,)), dma((2,)), dma((whole + 2,)), dma((steps, 2)), dma((steps, 2)), dma((steps - 1, whole + 2)),
            dma((3,)), dma((whole + 3,)), dma((2,)), dma((whole - lay.kept + 2,)),
            dma((3 + 2 * GROUP,)), dma((3 + 2 * GROUP,)), dma((2,)), dma((2,)),
        ],
        compiler_params=pltpu.CompilerParams(collective_id=0, has_side_effects=True, vmem_limit_bytes=54 * 2**20 - 84 * 2**10),
        name="distill",
    )(embedding.T, teacher_logits.T, hidden)
    peak, total, weight, cross = (sums.reshape(2, 4, -1)[:, k].reshape(-1) for k in range(4))
    norm_log = jnp.log(total)
    return peak + norm_log - cross / weight, -norm_log


def solution(mesh):
    sizes = [mesh.shape[name] for name in ("row", "col", "depth")]
    in_specs = (P("row", ("depth", "col")), P("col", ("depth", "row")), P("row", ("col", "depth")))
    out_specs = (P("row"), P("row"))
    return jax.shard_map(
        functools.partial(on_device, *sizes), mesh=mesh, in_specs=in_specs, out_specs=out_specs, check_vma=False
    )
```

```python
import functools

import jax
import jax.numpy as jnp
from jax import lax
from jax.experimental import pallas as pl
from jax.experimental.pallas import tpu as pltpu
from jax.sharding import PartitionSpec as P

MESH = pl.DeviceIdType.MESH
GROUP = 2
LANE = 128
CHUNK = 384
KEPT = 0.67
LOW = -1e30


class Layout:
    def __init__(self, vocab, depths):
        self.half = vocab // depths
        self.stride = vocab // LANE // (depths * GROUP) * LANE
        self.shift = self.half - GROUP * self.stride
        self.last = self.half - (GROUP - 1) * self.stride
        self.edge = ((self.stride - LANE) // CHUNK - 1) * CHUNK
        self.whole = self.edge // CHUNK
        self.plain = self.stride - self.edge
        self.tiles = self.plain // LANE
        self.rest = self.plain + LANE // 2
        self.kept = round(self.stride / CHUNK * KEPT)
        assert depths == 2 and 0 <= self.shift < CHUNK and self.shift % 16 == 0
        assert self.last + self.shift <= self.stride + LANE // 2 and self.plain % LANE == 0
        assert vocab <= self.stride * depths * GROUP + LANE // 2


def place():
    r, c, d = lax.axis_index("row"), lax.axis_index("col"), lax.axis_index("depth")
    return r, c, d, r // GROUP, lax.rem(r, GROUP)


def ends(rows, q):
    steps = rows // GROUP
    low, high = q == 0, q == steps - 1
    return low | high, (q == 1) | (q == steps - 2), jnp.where(q * 2 < steps, GROUP, -GROUP)


def as_count(flag):
    return flag.astype(jnp.int32)


def loop(begin, stop, body):
    def step(i, _):
        body(i)
        return 0

    lax.fori_loop(begin, stop, step, 0)


def gather_terms(parts):
    top, total, teacher_top, teacher_total, cross = parts
    peak = jnp.max(top, axis=0, keepdims=True)
    teacher_peak = jnp.max(teacher_top, axis=0, keepdims=True)
    scale = jnp.exp(teacher_top - teacher_peak)
    weight = jnp.sum(teacher_total * scale, axis=0, keepdims=True)
    return [
        peak,
        jnp.sum(total * jnp.exp(top - peak), axis=0, keepdims=True),
        teacher_peak + jnp.log(weight),
        jnp.sum(cross * scale, axis=0, keepdims=True) / weight,
    ]


def fold(values):
    whole = jnp.concatenate(values, axis=0)
    half = whole.shape[1] // 2
    return jnp.concatenate([whole[:, :half], whole[:, half:]], axis=0)


def product(rows, hidden):
    return lax.dot_general(rows, hidden, (((0,), (0,)), ((), ())), preferred_element_type=jnp.float32)


def add_terms(student, acc, at, teacher, valid=None):
    size = student.shape[0]
    teacher = teacher.astype(jnp.float32)
    if valid is not None:
        index = lax.broadcasted_iota(jnp.int32, student.shape, 0)
        keep = (index >= valid[0]) & (index < valid[1])
        student = jnp.where(keep, student, LOW)
        teacher = jnp.where(keep, teacher, LOW)
    student = student.reshape(size // 8, 8, -1)
    teacher = teacher.reshape(size // 8, 8, -1)
    old, teacher_old = acc[0, :, at], acc[2, :, at]
    top = jnp.maximum(old, jnp.max(student, axis=0))
    acc[1, :, at] = acc[1, :, at] * jnp.exp(old - top) + jnp.sum(jnp.exp(student - top[None]), axis=0)
    acc[0, :, at] = top
    teacher_top = jnp.maximum(teacher_old, jnp.max(teacher, axis=0))
    fade = jnp.exp(teacher_old - teacher_top)
    weights = jnp.exp(teacher - teacher_top[None])
    acc[3, :, at] = acc[3, :, at] * fade + jnp.sum(weights, axis=0)
    acc[4, :, at] = acc[4, :, at] * fade + jnp.sum(weights * student, axis=0)
    acc[2, :, at] = teacher_top


def kernel(
    rows, cols, depths, lay, emb_ref, teacher_ref, hidden_ref, sums_ref,
    table_ref, pack_ref, full_ref, half_ref, own_ref, other_ref, extra_ref, hid_ref, acc, ahead_ref, stats_ref, held_ref,
    own_sem, first_send, first_recv, right_send, left_send, line_recv, teach_send, teach_recv, extra_send, extra_recv,
    hid_send, hid_recv, stats_send, stats_recv,
):
    r, c, d, q, j = place()
    steps = rows // GROUP
    count = depths * GROUP
    me = d * GROUP + j
    kept, whole, edge = lay.kept, lay.whole, lay.edge
    narrow = table_ref.shape[0]
    packed = narrow // 2
    tokens = hidden_ref.shape[1]
    end, server, inward = ends(rows, q)
    pj = lax.rem(j + 1, GROUP)
    pr = q * GROUP + pj
    slice_ = d * cols + c
    peers = []
    for dj in range(GROUP):
        for dc in range(cols):
            for dd in range(depths):
                if dj or dc or dd:
                    peers.append((q * GROUP + lax.rem(j + dj, GROUP), lax.rem(c + dc, cols), lax.rem(d + dd, depths), dj))
    group = [(r, c, d, 0)] + peers
    near = len(peers)
    same = [(a, b, e) for a, b, e, dj in peers if dj == 0]

    barrier = pltpu.get_barrier_semaphore()

    def greet(row, col, depth):
        pl.semaphore_signal(barrier, inc=1, device_id=(row, col, depth), device_id_type=MESH)

    @pl.when(q + 1 < steps)
    def _():
        greet(r + GROUP, c, d)

    @pl.when(q > 0)
    def _():
        greet(r - GROUP, c, d)

    for a, b, e, _ in peers:
        greet(a, b, e)

    def remote(source_ref, dst_ref, send_sem, recv_sem, device):
        return pltpu.make_async_remote_copy(
            src_ref=source_ref, dst_ref=dst_ref, send_sem=send_sem, recv_sem=recv_sem, device_id=device, device_id_type=MESH
        )

    load = pltpu.make_async_copy(emb_ref, table_ref, own_sem.at[0])
    load.start()
    load.wait()
    for target in range(count):
        part = table_ref[:, lay.stride * (target + 1) : lay.stride * (target + 1) + LANE // 2]
        pack_ref[target] = jnp.concatenate([part[:packed], part[packed:]], axis=1)

    def span(t):
        return pl.multiple_of(t * CHUNK, CHUNK), CHUNK, t, narrow

    def tile_span(i):
        return pl.multiple_of(edge + i * LANE, LANE), LANE, whole + i, narrow

    half_span = (lay.stride, LANE, whole + lay.tiles, packed)
    ends_of = tuple(tile_span(i) for i in range(lay.tiles)) + (half_span,)

    def piece(target, cut):
        first_lane, size, index, height = cut
        if height != narrow:
            return pack_ref.at[target]
        return table_ref.at[:, pl.ds(pl.multiple_of(lay.stride * target + first_lane, LANE), size)]

    def slot(depth, row, cut):
        first_lane, size, _, height = cut
        return full_ref.at[depth, row, :, pl.ds(first_lane, size)] if height == narrow else half_ref.at[depth, row]

    def block_at(block, cut):
        first_lane, size, _, height = cut
        row = pl.ds(pl.multiple_of(block * GROUP, GROUP), GROUP)
        return full_ref.at[:, row, :, pl.ds(first_lane, size)] if height == narrow else half_ref.at[:, row]

    own_piece = pltpu.make_async_copy(
        table_ref.at[:, pl.ds(pl.multiple_of(lay.stride * me, LANE), lay.stride)],
        full_ref.at[d, r], own_sem.at[1],
    )
    own_half = pltpu.make_async_copy(pack_ref.at[me], slot(d, r, half_span), own_sem.at[2])

    def kind(cut):
        return 0 if cut[3] == narrow else 1

    def first(cut, off):
        target = lax.rem(me + off, count)
        return remote(
            piece(target, cut), slot(d, r, cut), first_send.at[kind(cut)], first_recv.at[cut[2]],
            (q * GROUP + lax.rem(target, GROUP), c, target // GROUP),
        )

    def first_arrived(cut):
        row = pl.ds(0, count - 1)
        at = full_ref.at[0, row, :, pl.ds(cut[0], cut[1])] if cut[3] == narrow else half_ref.at[0, row]
        return remote(at, at, first_send.at[0], first_recv.at[cut[2]], (pr, c, d))

    def send_line(source_ref, dst_ref, block, cut, right):
        sems, place_ = (right_send, block) if right else (left_send, block - 1)
        return remote(
            source_ref, dst_ref, sems.at[block, kind(cut)], line_recv.at[place_, cut[2]],
            (r + GROUP if right else r - GROUP, c, d),
        )

    def along(block, cut, right):
        at = block_at(block, cut)
        return send_line(at, at, block, cut, right)

    def arrived(block, cut, right):
        at = block_at(block, cut)
        return remote(at, at, right_send.at[0, 0], line_recv.at[block if right else block - 1, cut[2]], (pr, c, d))

    def to_right(t):
        return (q + 1 < steps) & ((t < kept) | (q + 2 < steps))

    def to_left(t):
        return (q > 0) & ((t < kept) | (q > 1))

    def both(cut, source_ref, dst_ref):
        @pl.when(to_right(cut[2]))
        def _():
            send_line(source_ref, dst_ref, q, cut, True).start()

        @pl.when(to_left(cut[2]))
        def _():
            send_line(source_ref, dst_ref, q, cut, False).start()

    def hidden_at(n, where=None):
        return hid_ref.at[slice_ if where is None else where, :, pl.ds(n * tokens, tokens)]

    def give(n, sem, device, source_ref):
        return remote(source_ref, hidden_at(n), hid_send.at[sem], hid_recv.at[sem], device)

    cross = [give(1, 0, (pr, c, d), hidden_ref), None, give(3, 1, (pr, c, d), hidden_at(2))]
    far_hid = give(2, 2, (r + inward, c, d), hidden_ref)
    spread = [
        [give(n, 3 + n, device, hidden_ref if n == 0 else hidden_at(n)) for device in same] for n in range(2 * GROUP)
    ]

    def spread_all(n):
        at = hidden_at(n, pl.ds(0, len(same)))
        return remote(at, at, hid_send.at[3 + n], hid_recv.at[3 + n], (pr, c, d))

    pl.semaphore_wait(barrier, near + as_count(q + 1 < steps) + as_count(q > 0))

    @pl.when(end)
    def _():
        far_hid.start()

    def launch(cut):
        both(cut, piece(me, cut), slot(d, r, cut))
        for off in range(1, count):
            first(cut, off).start()

    loop(0, whole, lambda t: launch(span(t)))
    for cut in ends_of:
        launch(cut)

    cross[0].start()
    for copy in spread[0]:
        copy.start()

    has_head = ~((d > 0) & (j == 0))
    peer_head = ~((d > 0) & (pj == 0))
    has_tail = (d == depths - 1) & (j == GROUP - 1)
    peer_tail = (d == depths - 1) & (pj == GROUP - 1)
    shift = lay.shift * (depths - 1)

    def source(part, at, size):
        begin = jnp.clip(lay.stride * part - lay.shift * d + at, 0, lay.half - size)
        return teacher_ref.at[pl.ds(pl.multiple_of(begin, 16), size)]

    own_body = pltpu.make_async_copy(source(j, shift, lay.last - shift), own_ref.at[pl.ds(shift, lay.last - shift)], own_sem.at[3])
    own_head = pltpu.make_async_copy(source(j, 0, shift), own_ref.at[pl.ds(0, shift)], own_sem.at[4])
    own_tail = pltpu.make_async_copy(source(j, lay.last, shift), own_ref.at[pl.ds(lay.last, shift)], own_sem.at[5])
    own_hid = pltpu.make_async_copy(hidden_ref, hidden_at(0), own_sem.at[6])
    own_piece.start()
    own_half.start()
    own_hid.start()
    own_body.start()

    @pl.when(has_head)
    def _():
        own_head.start()

    @pl.when(has_tail)
    def _():
        own_tail.start()

    @pl.when(server)
    def _():
        far_hid.wait_recv()
        cross[2].start()
        for copy in spread[2]:
            copy.start()

    def start_line(cut):
        first_arrived(cut).wait_recv()
        for off in range(1, count):
            sender = lax.rem(me + count - off, count)
            at = slot(sender // GROUP, q * GROUP + lax.rem(sender, GROUP), cut)
            both(cut, at, at)


    body = lay.last - edge

    def teach_rows(index, at, size, sem=0):
        return remote(source(pj, at, size), other_ref.at[pl.ds(at, size)], teach_send.at[sem], teach_recv.at[index], (pr, c, d))

    def teach(t):
        return teach_rows(t, pl.multiple_of(t * CHUNK, CHUNK), CHUNK)

    teach_zero = teach_rows(0, shift, CHUNK - shift)
    teach_head = teach_rows(whole + 1, 0, shift, 1)
    teach_body = teach_rows(whole, edge, body)
    teach_tail = teach_rows(whole + 2, lay.last, shift, 2)

    def teach_kept():
        teach_zero.start()

        @pl.when(peer_head)
        def _():
            teach_head.start()

        loop(1, kept, lambda t: teach(t).start())

    def teach_rest():
        loop(kept, whole, lambda t: teach(t).start())
        teach_body.start()

        @pl.when(peer_tail)
        def _():
            teach_tail.start()

    loop(0, whole * 3 // 4, lambda t: start_line(span(t)))

    @pl.when(end)
    def _():
        teach_rest()

    teach_kept()

    @pl.when(~end)
    def _():
        teach_rest()

    loop(whole * 3 // 4, whole, lambda t: start_line(span(t)))
    for cut in ends_of:
        start_line(cut)

    cross[0].wait_recv()
    for copy in spread[1]:
        copy.start()

    @pl.when(server)
    def _():
        cross[2].wait_recv()
        for copy in spread[3]:
            copy.start()

    def teach_end_arrived():
        teach_body.wait_recv()

        @pl.when(has_tail)
        def _():
            teach_tail.wait_recv()

    base = kept * CHUNK

    def extra_rows(n, index, at, size, sem=0):
        return remote(
            source(j, at, size) if n == 0 else other_ref.at[pl.ds(at, size)],
            extra_ref.at[n, pl.ds(at - base, size)], extra_send.at[sem], extra_recv.at[index], (r + inward, c, d),
        )

    def extra_arrived(index, at, size, sem=0):
        both_sets = extra_ref.at[:, pl.ds(at - base, size)]
        return remote(both_sets, both_sets, extra_send.at[sem], extra_recv.at[index], (pr, c, d))

    def extra_at(t):
        return t - kept, pl.multiple_of(t * CHUNK, CHUNK), CHUNK

    extra_body = (whole - kept, edge, body)
    extra_tail = (whole - kept + 1, lay.last, shift, 1)

    @pl.when(end)
    def _():
        def pass_on(t):
            teach(t).wait_recv()
            for n in range(GROUP):
                extra_rows(n, *extra_at(t)).start()

        loop(kept, whole, pass_on)
        teach_end_arrived()
        for n in range(GROUP):
            extra_rows(n, *extra_body).start()

        @pl.when(has_tail)
        def _():
            for n in range(GROUP):
                extra_rows(n, *extra_tail).start()

    def hop(k, cut):
        t = cut[2]
        wanted = (t < kept) | ~end

        @pl.when((q - k >= 0) & wanted)
        def _():
            arrived(q - k, cut, True).wait_recv()

            @pl.when(to_right(t))
            def _():
                along(q - k, cut, True).start()

        @pl.when((q + k < steps) & wanted)
        def _():
            arrived(q + k, cut, False).wait_recv()

            @pl.when(to_left(t))
            def _():
                along(q + k, cut, False).start()

    far = jnp.maximum(q, steps - 1 - q)

    def early(k):
        loop(0, whole, lambda t: hop(k, span(t)))
        for cut in ends_of:
            hop(k, cut)

    loop(1, far, early)

    for k in range(5):
        acc[k] = jnp.full(acc.shape[1:], LOW if k in (0, 2) else 0.0, jnp.float32)

    def features(t):
        return full_ref[:, :, :, pl.ds(pl.multiple_of(t * CHUNK, CHUNK), CHUNK)].reshape(-1, CHUNK)

    def token_lanes(sets):
        return pl.ds(sets[0] * tokens, len(sets) * tokens)

    def hidden_of(sets):
        return hid_ref[:, :, token_lanes(sets)].reshape(-1, len(sets) * tokens)

    def unpacked(half):
        half = jnp.concatenate([half[..., : LANE // 2], half[..., LANE // 2 :]], axis=2)
        return half.reshape(-1, LANE // 2)

    def tile_features(begin, size, block=None):
        at = pl.ds(0, rows) if block is None else pl.ds(block * GROUP, GROUP)
        return full_ref[:, at, :, pl.ds(begin, size)].reshape(-1, size)

    def half_features(block=None):
        return unpacked(half_ref[:, pl.ds(0, rows) if block is None else pl.ds(block * GROUP, GROUP)])

    def hidden_block(block, sets):
        begin = block * (GROUP * narrow)
        at = pl.ds(pl.multiple_of(lax.rem(begin, hid_ref.shape[1]), 16), GROUP * narrow)
        parts = [hid_ref[depth * cols + begin // hid_ref.shape[1], at, token_lanes(sets)] for depth in range(depths)]
        return jnp.concatenate(parts, axis=0)

    def main(rows_, at, valid=None):
        for n, ref in enumerate((own_ref, other_ref)):
            add_terms(product(rows_, hidden_of((n,))), acc, token_lanes((n,)), ref[at, :], valid)

    def more(rows_, at):
        for n in range(GROUP):
            add_terms(product(rows_, hidden_of((GROUP + n,))), acc, token_lanes((GROUP + n,)), extra_ref[n, at, :])

    def teacher_of(sets, begin, size):
        at = pl.ds(begin, size)
        own = [own_ref[at, :], other_ref[at, :]]
        taken = [extra_ref[n, pl.ds(pl.multiple_of(begin - base, LANE // 2), size), :] for n in range(GROUP)] if len(sets) > GROUP else []
        return jnp.concatenate(own + taken, axis=1)

    ahead = steps <= 4 and narrow % 32 == 16 and hid_ref.shape[1] % (GROUP * narrow) == 0
    last_block = jnp.where(q * 2 < steps, steps - 1, 0)

    def prepare(sets):
        if not ahead:
            return
        at = token_lanes(sets)
        tiles, half_rows = pl.ds(0, lay.plain), pl.ds(lay.plain, LANE // 2)
        for n in range(1, steps):
            block = lax.rem(last_block + n, steps)
            hidden = hidden_block(block, sets)
            tile = product(tile_features(edge, lay.plain, block), hidden)
            half = product(half_features(block), hidden)
            ahead_ref[tiles, at] = tile if n == 1 else ahead_ref[tiles, at] + tile
            ahead_ref[half_rows, at] = half if n == 1 else ahead_ref[half_rows, at] + half

    def end_student(sets, take, begin, size):
        if not ahead:
            return product(take(), hidden_of(sets))
        return ahead_ref[pl.ds(begin, size), token_lanes(sets)] + product(take(last_block), hidden_block(last_block, sets))

    def rows_at(t):
        return pl.ds(pl.multiple_of(t * CHUNK, CHUNK), CHUNK)

    hop(far, span(0))
    own_body.wait()

    @pl.when(has_head)
    def _():
        own_head.wait()

    @pl.when(has_tail)
    def _():
        own_tail.wait()

    own_hid.wait()
    own_piece.wait()
    own_half.wait()
    for n in range(2):
        spread_all(n).wait_recv()
    teach_zero.wait_recv()

    @pl.when(has_head)
    def _():
        teach_head.wait_recv()

    main(features(0), rows_at(0), (jnp.where(has_head, 0, shift), CHUNK))

    def kept_chunk(t):
        hop(far, span(t))
        teach(t).wait_recv()
        main(features(t), rows_at(t))

    loop(1, kept, kept_chunk)

    @pl.when(server)
    def _():
        for n in range(2, 4):
            spread_all(n).wait_recv()

    @pl.when(~end)
    def _():
        def rest_chunk(t):
            hop(far, span(t))

            teach(t).wait_recv()
            main(features(t), rows_at(t))

            @pl.when(server)
            def _():
                extra_arrived(*extra_at(t)).wait_recv()
                more(features(t), rows_at(t - kept))

        loop(kept, whole - 1, rest_chunk)

        @pl.when(server)
        def _():
            prepare(tuple(range(2 * GROUP)))

        @pl.when(~server)
        def _():
            prepare(tuple(range(GROUP)))

        rest_chunk(whole - 1)

    def close(sets):
        at = pl.ds(sets[0] * tokens, len(sets) * tokens)
        values = gather_terms([acc[k, :, at] for k in range(5)])
        for n in range(len(sets)):
            stats_ref[sets[n]] = fold([value[:, n * tokens : (n + 1) * tokens] for value in values])

    def tell(n, sem, device, source_set):
        return remote(stats_ref.at[source_set], held_ref.at[n], stats_send.at[sem], stats_recv.at[sem], device)

    def told(sem, begin, size):
        at = held_ref.at[pl.ds(begin, size)]
        return remote(at, at, stats_send.at[sem], stats_recv.at[sem], (pr, c, d))

    limit = (0, lay.last + lay.shift * d - lay.stride)
    half_used = j == GROUP - 1

    own_sets, all_sets = tuple(range(GROUP)), tuple(range(2 * GROUP))

    def tell_near():
        for n, (a, b, e, dj) in reversed(list(enumerate(peers))):
            tell(n, 0, (a, b, e), dj).start()

    def finish(sets):
        at = token_lanes(sets)

        def tile_terms(i):
            cut = tile_span(i)
            hop(far, cut)
            take = functools.partial(tile_features, cut[0], LANE)
            student = end_student(sets, take, pl.multiple_of(i * LANE, LANE), LANE)
            add_terms(student, acc, at, teacher_of(sets, cut[0], LANE))

        loop(0, lay.tiles, tile_terms)
        hop(far, half_span)

        @pl.when(half_used)
        def _():
            student = end_student(sets, half_features, lay.plain, LANE // 2)
            add_terms(student, acc, at, teacher_of(sets, lay.stride, LANE // 2), limit)

        close(sets)

    @pl.when(~end)
    def _():
        teach_end_arrived()

    @pl.when(server)
    def _():
        extra_arrived(*extra_body).wait_recv()

        @pl.when(has_tail)
        def _():
            extra_arrived(*extra_tail).wait_recv()

        finish(all_sets)
        for n, (a, b, e, dj) in reversed(list(enumerate(group))):
            tell(near + n, 1, (a - inward, b, e), GROUP + dj).start()

    @pl.when(~end & ~server)
    def _():
        finish(own_sets)

    @pl.when(end)
    def _():
        close(own_sets)

    tell_near()

    @pl.when(~end)
    def _():
        kinds = lax.broadcasted_iota(jnp.int32, held_ref.shape[1:], 0) % 2
        for n in range(len(group)):
            held_ref[near + n] = jnp.where(kinds == 0, LOW, 0.0)

    def settle(block):
        def sent(right, size):
            at = block_at(block, (0, size, 0, narrow))
            remote(at, at, (right_send if right else left_send).at[block, 0], line_recv.at[0, 0], (pr, c, d)).wait_send()

        def sent_half(right):
            at = block_at(block, half_span)
            remote(at, at, (right_send if right else left_send).at[block, 1], line_recv.at[0, 0], (pr, c, d)).wait_send()

        @pl.when((block <= q) & (q + 2 < steps))
        def _():
            sent(True, lay.stride)
            sent_half(True)

        @pl.when((block <= q) & (q + 2 == steps))
        def _():
            sent(True, base)

        @pl.when((block >= q) & (q > 1))
        def _():
            sent(False, lay.stride)
            sent_half(False)

        @pl.when((block >= q) & (q == 1))
        def _():
            sent(False, base)

    loop(0, steps, settle)
    sent_pieces = full_ref.at[0, pl.ds(0, count - 1)]
    remote(sent_pieces, sent_pieces, first_send.at[0], first_recv.at[0], (pr, c, d)).wait_send()
    sent_halves = half_ref.at[0, pl.ds(0, count - 1)]
    remote(sent_halves, sent_halves, first_send.at[1], first_recv.at[0], (pr, c, d)).wait_send()
    cross[0].wait_send()
    for n in range(2):
        spread_all(n).wait_send()
    taught = other_ref.at[pl.ds(shift, lay.last - shift)]
    remote(taught, taught, teach_send.at[0], teach_recv.at[0], (pr, c, d)).wait_send()

    @pl.when(peer_head)
    def _():
        teach_head.wait_send()

    @pl.when(peer_tail)
    def _():
        teach_tail.wait_send()

    @pl.when(end)
    def _():
        far_hid.wait_send()
        extra_arrived(0, base, lay.last - base).wait_send()

        @pl.when(has_tail)
        def _():
            extra_arrived(*extra_tail).wait_send()

    @pl.when(server)
    def _():
        cross[2].wait_send()
        for n in range(2, 4):
            spread_all(n).wait_send()
        told(1, near, len(group)).wait_send()

    told(0, 0, near).wait()

    @pl.when(end)
    def _():
        told(1, near, len(group)).wait_recv()

    blocks = [stats_ref[0]] + [held_ref[n] for n in range(near + len(group))]
    top = functools.reduce(jnp.maximum, blocks)
    scales = [jnp.exp(block - top) for block in blocks]
    weight = functools.reduce(jnp.add, scales)
    scaled = functools.reduce(jnp.add, [block * pltpu.roll(scale, 1, 0) for block, scale in zip(blocks, scales)])
    row_kind = lax.broadcasted_iota(jnp.int32, top.shape, 0) % 4
    sums_ref[...] = jnp.where(row_kind == 0, top, jnp.where(row_kind == 2, weight, scaled))


def on_device(rows, cols, depths, student_hidden, embedding, teacher_logits):
    vocab, narrow = embedding.shape
    lay = Layout(vocab, depths)
    hidden = student_hidden.T
    features, tokens = hidden.shape
    steps = rows // GROUP
    slots = 2 * GROUP * cols * depths - 1
    whole, height = lay.whole, lay.edge + lay.rest
    dma = pltpu.SemaphoreType.DMA
    any_space = pl.BlockSpec(memory_space=pl.ANY)
    dtype = embedding.dtype
    sums = pl.pallas_call(
        functools.partial(kernel, rows, cols, depths, lay),
        out_shape=jax.ShapeDtypeStruct((8, tokens // 2), jnp.float32),
        in_specs=[any_space] * 3,
        out_specs=pl.BlockSpec(memory_space=pltpu.VMEM),
        scratch_shapes=[
            pltpu.VMEM((narrow, vocab), dtype),
            pltpu.VMEM((depths * GROUP, narrow // 2, LANE), dtype),
            pltpu.VMEM((depths, rows, narrow, lay.stride), dtype),
            pltpu.VMEM((depths, rows, narrow // 2, LANE), dtype),
            pltpu.VMEM((height, tokens), teacher_logits.dtype),
            pltpu.VMEM((height, tokens), teacher_logits.dtype),
            pltpu.VMEM((GROUP, height - lay.kept * CHUNK, tokens), teacher_logits.dtype),
            pltpu.VMEM((depths * cols, features, 2 * GROUP * tokens), hidden.dtype),
            pltpu.VMEM((5, 8, 2 * GROUP * tokens), jnp.float32),
            pltpu.VMEM((lay.rest, 2 * GROUP * tokens), jnp.float32),
            pltpu.VMEM((2 * GROUP, 8, tokens // 2), jnp.float32),
            pltpu.VMEM((slots, 8, tokens // 2), jnp.float32),
            dma((7,)), dma((2,)), dma((whole + lay.tiles + 1,)), dma((steps, 2)), dma((steps, 2)), dma((steps - 1, whole + lay.tiles + 1)),
            dma((3,)), dma((whole + 3,)), dma((2,)), dma((whole - lay.kept + 2,)),
            dma((3 + 2 * GROUP,)), dma((3 + 2 * GROUP,)), dma((2,)), dma((2,)),
        ],
        compiler_params=pltpu.CompilerParams(collective_id=0, has_side_effects=True, vmem_limit_bytes=54 * 2**20 - 84 * 2**10),
        name="distill",
    )(embedding.T, teacher_logits.T, hidden)
    peak, total, weight, cross = (sums.reshape(2, 4, -1)[:, k].reshape(-1) for k in range(4))
    norm_log = jnp.log(total)
    return peak + norm_log - cross / weight, -norm_log


def solution(mesh):
    sizes = [mesh.shape[name] for name in ("row", "col", "depth")]
    in_specs = (P("row", ("depth", "col")), P("col", ("depth", "row")), P("row", ("col", "depth")))
    out_specs = (P("row"), P("row"))
    return jax.shard_map(
        functools.partial(on_device, *sizes), mesh=mesh, in_specs=in_specs, out_specs=out_specs, check_vma=False
    )
```

```python
import functools

import jax
import jax.numpy as jnp
from jax import lax
from jax.experimental import pallas as pl
from jax.experimental.pallas import tpu as pltpu
from jax.sharding import PartitionSpec as P

MESH = pl.DeviceIdType.MESH
GROUP = 2
LANE = 128
CHUNK = 384
KEPT = 0.67
LOW = -1e30


class Layout:
    def __init__(self, vocab, depths):
        self.half = vocab // depths
        self.stride = vocab // LANE // (depths * GROUP) * LANE
        self.shift = self.half - GROUP * self.stride
        self.last = self.half - (GROUP - 1) * self.stride
        self.edge = ((self.stride - LANE) // CHUNK - 1) * CHUNK
        self.whole = self.edge // CHUNK
        self.plain = self.stride - self.edge
        self.tiles = self.plain // LANE
        self.rest = self.plain + LANE // 2
        self.kept = round(self.stride / CHUNK * KEPT)
        assert depths == 2 and GROUP == 2 and 0 <= self.shift < CHUNK and self.shift % 16 == 0
        assert self.last + self.shift <= self.stride + LANE // 2 and self.plain % LANE == 0
        assert vocab <= self.stride * depths * GROUP + LANE // 2


def place():
    r, c, d = lax.axis_index("row"), lax.axis_index("col"), lax.axis_index("depth")
    return r, c, d, r // GROUP, lax.rem(r, GROUP)


def ends(rows, q):
    steps = rows // GROUP
    low, high = q == 0, q == steps - 1
    return low | high, (q == 1) | (q == steps - 2), jnp.where(q * 2 < steps, GROUP, -GROUP)


def as_count(flag):
    return flag.astype(jnp.int32)


def loop(begin, stop, body):
    def step(i, _):
        body(i)
        return 0

    lax.fori_loop(begin, stop, step, 0)


def gather_terms(parts):
    top, total, teacher_top, teacher_total, cross = parts
    peak = jnp.max(top, axis=0, keepdims=True)
    teacher_peak = jnp.max(teacher_top, axis=0, keepdims=True)
    scale = jnp.exp(teacher_top - teacher_peak)
    weight = jnp.sum(teacher_total * scale, axis=0, keepdims=True)
    return [
        peak,
        jnp.sum(total * jnp.exp(top - peak), axis=0, keepdims=True),
        teacher_peak + jnp.log(weight),
        jnp.sum(cross * scale, axis=0, keepdims=True) / weight,
    ]


def fold(values):
    whole = jnp.concatenate(values, axis=0)
    half = whole.shape[1] // 2
    return jnp.concatenate([whole[:, :half], whole[:, half:]], axis=0)


def product(rows, hidden):
    return lax.dot_general(rows, hidden, (((0,), (0,)), ((), ())), preferred_element_type=jnp.float32)


def add_terms(student, acc, at, teacher, valid=None):
    size = student.shape[0]
    teacher = teacher.astype(jnp.float32)
    if valid is not None:
        index = lax.broadcasted_iota(jnp.int32, student.shape, 0)
        keep = (index >= valid[0]) & (index < valid[1])
        student = jnp.where(keep, student, LOW)
        teacher = jnp.where(keep, teacher, LOW)
    student = student.reshape(size // 8, 8, -1)
    teacher = teacher.reshape(size // 8, 8, -1)
    old, teacher_old = acc[0, :, at], acc[2, :, at]
    top = jnp.maximum(old, jnp.max(student, axis=0))
    acc[1, :, at] = acc[1, :, at] * jnp.exp(old - top) + jnp.sum(jnp.exp(student - top[None]), axis=0)
    acc[0, :, at] = top
    teacher_top = jnp.maximum(teacher_old, jnp.max(teacher, axis=0))
    fade = jnp.exp(teacher_old - teacher_top)
    weights = jnp.exp(teacher - teacher_top[None])
    acc[3, :, at] = acc[3, :, at] * fade + jnp.sum(weights, axis=0)
    acc[4, :, at] = acc[4, :, at] * fade + jnp.sum(weights * student, axis=0)
    acc[2, :, at] = teacher_top


def kernel(
    rows, cols, depths, lay, emb_ref, teacher_ref, hidden_ref, sums_ref,
    table_ref, pack_ref, full_ref, half_ref, own_ref, other_ref, extra_ref, hid_ref, acc, ahead_ref, stats_ref, held_ref,
    own_sem, first_send, first_recv, right_send, left_send, line_recv, teach_send, teach_recv, extra_send, extra_recv,
    hid_send, hid_recv, stats_send, stats_recv,
):
    r, c, d, q, j = place()
    steps = rows // GROUP
    count = depths * GROUP
    me = d * GROUP + j
    kept, whole, edge = lay.kept, lay.whole, lay.edge
    narrow = table_ref.shape[0]
    packed = narrow // 2
    tokens = hidden_ref.shape[1]
    end, server, inward = ends(rows, q)
    pj = lax.rem(j + 1, GROUP)
    pr = q * GROUP + pj
    slice_ = d * cols + c
    peers = []
    for dj in range(GROUP):
        for dc in range(cols):
            for dd in range(depths):
                if dj or dc or dd:
                    peers.append((q * GROUP + lax.rem(j + dj, GROUP), lax.rem(c + dc, cols), lax.rem(d + dd, depths), dj))
    group = [(r, c, d, 0)] + peers
    near = len(peers)
    same = [(a, b, e) for a, b, e, dj in peers if dj == 0]

    barrier = pltpu.get_barrier_semaphore()

    def greet(row, col, depth):
        pl.semaphore_signal(barrier, inc=1, device_id=(row, col, depth), device_id_type=MESH)

    @pl.when(q + 1 < steps)
    def _():
        greet(r + GROUP, c, d)

    @pl.when(q > 0)
    def _():
        greet(r - GROUP, c, d)

    greet(pr, c, d)
    greet(r, lax.rem(c + 1, cols), d)
    greet(r, c, lax.rem(d + 1, depths))

    def remote(source_ref, dst_ref, send_sem, recv_sem, device):
        return pltpu.make_async_remote_copy(
            src_ref=source_ref, dst_ref=dst_ref, send_sem=send_sem, recv_sem=recv_sem, device_id=device, device_id_type=MESH
        )

    load = pltpu.make_async_copy(emb_ref, table_ref, own_sem.at[0])
    strip = 8 if narrow % 8 == 0 else narrow
    for at in range(0, narrow, strip):
        rows_ = pl.ds(at, strip)
        pltpu.make_async_copy(emb_ref.at[rows_], table_ref.at[rows_], own_sem.at[0]).start()
    load.wait()
    for target in range(count):
        part = table_ref[:, lay.stride * (target + 1) : lay.stride * (target + 1) + LANE // 2]
        pack_ref[target] = jnp.concatenate([part[:packed], part[packed:]], axis=1)

    def span(t):
        return pl.multiple_of(t * CHUNK, CHUNK), CHUNK, t, narrow

    def tile_span(i):
        return pl.multiple_of(edge + i * LANE, LANE), LANE, whole + i, narrow

    half_span = (lay.stride, LANE, whole + lay.tiles, packed)
    ends_of = tuple(tile_span(i) for i in range(lay.tiles)) + (half_span,)

    def piece(target, cut):
        first_lane, size, index, height = cut
        if height != narrow:
            return pack_ref.at[target]
        return table_ref.at[:, pl.ds(pl.multiple_of(lay.stride * target + first_lane, LANE), size)]

    def slot(depth, row, cut):
        first_lane, size, _, height = cut
        return full_ref.at[depth, row, :, pl.ds(first_lane, size)] if height == narrow else half_ref.at[depth, row]

    def block_at(block, cut):
        first_lane, size, _, height = cut
        row = pl.ds(pl.multiple_of(block * GROUP, GROUP), GROUP)
        return full_ref.at[:, row, :, pl.ds(first_lane, size)] if height == narrow else half_ref.at[:, row]

    own_piece = pltpu.make_async_copy(
        table_ref.at[:, pl.ds(pl.multiple_of(lay.stride * me, LANE), lay.stride)],
        full_ref.at[d, r], own_sem.at[1],
    )
    own_half = pltpu.make_async_copy(pack_ref.at[me], slot(d, r, half_span), own_sem.at[2])

    def kind(cut):
        return 0 if cut[3] == narrow else 1

    def first(cut, off):
        target = lax.rem(me + off, count)
        return remote(
            piece(target, cut), slot(d, r, cut), first_send.at[kind(cut)], first_recv.at[cut[2]],
            (q * GROUP + lax.rem(target, GROUP), c, target // GROUP),
        )

    def first_arrived(cut):
        row = pl.ds(0, count - 1)
        at = full_ref.at[0, row, :, pl.ds(cut[0], cut[1])] if cut[3] == narrow else half_ref.at[0, row]
        return remote(at, at, first_send.at[0], first_recv.at[cut[2]], (pr, c, d))

    def send_line(source_ref, dst_ref, block, cut, right):
        sems, place_ = (right_send, block) if right else (left_send, block - 1)
        return remote(
            source_ref, dst_ref, sems.at[block, kind(cut)], line_recv.at[place_, cut[2]],
            (r + GROUP if right else r - GROUP, c, d),
        )

    def along(block, cut, right):
        at = block_at(block, cut)
        return send_line(at, at, block, cut, right)

    def arrived(block, cut, right):
        at = block_at(block, cut)
        return remote(at, at, right_send.at[0, 0], line_recv.at[block if right else block - 1, cut[2]], (pr, c, d))

    half_used = j == GROUP - 1

    def uses(cut, flag):
        return flag if cut[3] == narrow else flag & half_used

    def to_right(t):
        return (q + 1 < steps) & ((t < kept) | (q + 2 < steps))

    def to_left(t):
        return (q > 0) & ((t < kept) | (q > 1))

    def both(cut, source_ref, dst_ref):
        @pl.when(uses(cut, to_right(cut[2])))
        def _():
            send_line(source_ref, dst_ref, q, cut, True).start()

        @pl.when(uses(cut, to_left(cut[2])))
        def _():
            send_line(source_ref, dst_ref, q, cut, False).start()

    def hidden_at(n, where=None):
        return hid_ref.at[slice_ if where is None else where, :, pl.ds(n * tokens, tokens)]

    def give(n, sem, device, source_ref):
        return remote(source_ref, hidden_at(n), hid_send.at[sem], hid_recv.at[sem], device)

    cross = [give(1, 0, (pr, c, d), hidden_ref), None, give(3, 1, (pr, c, d), hidden_at(2))]
    far_hid = give(2, 2, (r + inward, c, d), hidden_ref)
    spread = [
        [give(n, 3 + n, device, hidden_ref if n == 0 else hidden_at(n)) for device in same] for n in range(2 * GROUP)
    ]

    def spread_all(n):
        at = hidden_at(n, pl.ds(0, len(same)))
        return remote(at, at, hid_send.at[3 + n], hid_recv.at[3 + n], (pr, c, d))

    pl.semaphore_wait(barrier, 3 + as_count(q + 1 < steps) + as_count(q > 0))

    @pl.when(end)
    def _():
        far_hid.start()

    cross[0].start()
    by_x, by_y, by_both = GROUP, jnp.where(j == 0, 1, count - 1), jnp.where(j == 0, count - 1, 1)

    def launch_own(cut):
        both(cut, piece(me, cut), slot(d, r, cut))

    def launch_first(cut, off, ahead_):
        if cut[3] == narrow:
            first(cut, off).start()
            return

        @pl.when(half_used == ahead_)
        def _():
            first(cut, off).start()

    def launch_near(cut):
        launch_first(cut, by_y, False)
        launch_first(cut, by_x, True)

    def launch_far(cut):
        launch_first(cut, by_both, False)

    def opening(t):
        launch_own(span(t))
        launch_near(span(t))

    lead = min(4, whole)
    loop(0, lead, opening)
    loop(lead, whole, lambda t: launch_own(span(t)))
    for cut in ends_of:
        launch_own(cut)
    cross[0].wait_recv()

    def crossing(t):
        launch_far(span(t - lead))
        launch_near(span(t))

    loop(lead, whole, crossing)
    loop(whole - lead, whole, lambda t: launch_far(span(t)))
    for cut in ends_of:
        launch_near(cut)
        launch_far(cut)

    has_head = ~((d > 0) & (j == 0))
    peer_head = ~((d > 0) & (pj == 0))
    has_tail = (d == depths - 1) & (j == GROUP - 1)
    peer_tail = (d == depths - 1) & (pj == GROUP - 1)
    shift = lay.shift * (depths - 1)

    def source(part, at, size):
        begin = jnp.clip(lay.stride * part - lay.shift * d + at, 0, lay.half - size)
        return teacher_ref.at[pl.ds(pl.multiple_of(begin, 16), size)]

    own_body = pltpu.make_async_copy(source(j, shift, lay.last - shift), own_ref.at[pl.ds(shift, lay.last - shift)], own_sem.at[3])
    own_head = pltpu.make_async_copy(source(j, 0, shift), own_ref.at[pl.ds(0, shift)], own_sem.at[4])
    own_tail = pltpu.make_async_copy(source(j, lay.last, shift), own_ref.at[pl.ds(lay.last, shift)], own_sem.at[5])
    own_hid = pltpu.make_async_copy(hidden_ref, hidden_at(0), own_sem.at[6])
    own_piece.start()
    own_half.start()
    own_hid.start()
    own_body.start()

    @pl.when(has_head)
    def _():
        own_head.start()

    @pl.when(has_tail)
    def _():
        own_tail.start()

    @pl.when(server)
    def _():
        far_hid.wait_recv()
        cross[2].start()

    def start_line(cut):
        first_arrived(cut).wait_recv()
        for off in range(1, count):
            sender = lax.rem(me + count - off, count)
            at = slot(sender // GROUP, q * GROUP + lax.rem(sender, GROUP), cut)
            both(cut, at, at)


    body = lay.last - edge

    def teach_rows(index, at, size, sem=0):
        return remote(source(pj, at, size), other_ref.at[pl.ds(at, size)], teach_send.at[sem], teach_recv.at[index], (pr, c, d))

    def teach(t):
        return teach_rows(t, pl.multiple_of(t * CHUNK, CHUNK), CHUNK)

    teach_zero = teach_rows(0, shift, CHUNK - shift)
    teach_head = teach_rows(whole + 1, 0, shift, 1)
    teach_body = teach_rows(whole, edge, body)
    teach_tail = teach_rows(whole + 2, lay.last, shift, 2)

    def teach_kept():
        teach_zero.start()

        @pl.when(peer_head)
        def _():
            teach_head.start()

        loop(1, kept, lambda t: teach(t).start())

    def teach_rest():
        loop(kept, whole, lambda t: teach(t).start())
        teach_body.start()

        @pl.when(peer_tail)
        def _():
            teach_tail.start()

    loop(0, whole * 3 // 4, lambda t: start_line(span(t)))

    @pl.when(end)
    def _():
        teach_rest()

    teach_kept()

    @pl.when(~end)
    def _():
        teach_rest()

    loop(whole * 3 // 4, whole, lambda t: start_line(span(t)))
    for cut in ends_of[:-1]:
        start_line(cut)

    @pl.when(half_used)
    def _():
        start_line(half_span)

    for copy in spread[0] + spread[1]:
        copy.start()

    @pl.when(server)
    def _():
        cross[2].wait_recv()
        for copy in spread[2] + spread[3]:
            copy.start()

    def teach_end_arrived():
        teach_body.wait_recv()

        @pl.when(has_tail)
        def _():
            teach_tail.wait_recv()

    base = kept * CHUNK

    def extra_rows(n, index, at, size, sem=0):
        return remote(
            source(j, at, size) if n == 0 else other_ref.at[pl.ds(at, size)],
            extra_ref.at[n, pl.ds(at - base, size)], extra_send.at[sem], extra_recv.at[index], (r + inward, c, d),
        )

    def extra_arrived(index, at, size, sem=0):
        both_sets = extra_ref.at[:, pl.ds(at - base, size)]
        return remote(both_sets, both_sets, extra_send.at[sem], extra_recv.at[index], (pr, c, d))

    def extra_at(t):
        return t - kept, pl.multiple_of(t * CHUNK, CHUNK), CHUNK

    extra_body = (whole - kept, edge, body)
    extra_tail = (whole - kept + 1, lay.last, shift, 1)

    @pl.when(end)
    def _():
        def pass_on(t):
            teach(t).wait_recv()
            for n in range(GROUP):
                extra_rows(n, *extra_at(t)).start()

        loop(kept, whole, pass_on)
        teach_end_arrived()
        for n in range(GROUP):
            extra_rows(n, *extra_body).start()

        @pl.when(has_tail)
        def _():
            for n in range(GROUP):
                extra_rows(n, *extra_tail).start()

    def hop(k, cut):
        t = cut[2]
        wanted = uses(cut, (t < kept) | ~end)

        @pl.when((q - k >= 0) & wanted)
        def _():
            arrived(q - k, cut, True).wait_recv()

            @pl.when(to_right(t))
            def _():
                along(q - k, cut, True).start()

        @pl.when((q + k < steps) & wanted)
        def _():
            arrived(q + k, cut, False).wait_recv()

            @pl.when(to_left(t))
            def _():
                along(q + k, cut, False).start()

    far = jnp.maximum(q, steps - 1 - q)

    def early(k):
        loop(0, whole, lambda t: hop(k, span(t)))
        for cut in ends_of:
            hop(k, cut)

    loop(1, far, early)

    for k in range(5):
        acc[k] = jnp.full(acc.shape[1:], LOW if k in (0, 2) else 0.0, jnp.float32)

    def features(t):
        return full_ref[:, :, :, pl.ds(pl.multiple_of(t * CHUNK, CHUNK), CHUNK)].reshape(-1, CHUNK)

    def token_lanes(sets):
        return pl.ds(sets[0] * tokens, len(sets) * tokens)

    def hidden_of(sets):
        return hid_ref[:, :, token_lanes(sets)].reshape(-1, len(sets) * tokens)

    def unpacked(half):
        half = jnp.concatenate([half[..., : LANE // 2], half[..., LANE // 2 :]], axis=2)
        return half.reshape(-1, LANE // 2)

    def tile_features(begin, size, block=None):
        at = pl.ds(0, rows) if block is None else pl.ds(block * GROUP, GROUP)
        return full_ref[:, at, :, pl.ds(begin, size)].reshape(-1, size)

    def half_features(block=None):
        return unpacked(half_ref[:, pl.ds(0, rows) if block is None else pl.ds(block * GROUP, GROUP)])

    def hidden_block(block, sets):
        begin = block * (GROUP * narrow)
        at = pl.ds(pl.multiple_of(lax.rem(begin, hid_ref.shape[1]), 16), GROUP * narrow)
        parts = [hid_ref[depth * cols + begin // hid_ref.shape[1], at, token_lanes(sets)] for depth in range(depths)]
        return jnp.concatenate(parts, axis=0)

    def main(rows_, at, valid=None):
        for n, ref in enumerate((own_ref, other_ref)):
            add_terms(product(rows_, hidden_of((n,))), acc, token_lanes((n,)), ref[at, :], valid)

    def more(rows_, at):
        for n in range(GROUP):
            add_terms(product(rows_, hidden_of((GROUP + n,))), acc, token_lanes((GROUP + n,)), extra_ref[n, at, :])

    def teacher_of(sets, begin, size):
        at = pl.ds(begin, size)
        own = [own_ref[at, :], other_ref[at, :]]
        taken = [extra_ref[n, pl.ds(pl.multiple_of(begin - base, LANE // 2), size), :] for n in range(GROUP)] if len(sets) > GROUP else []
        return jnp.concatenate(own + taken, axis=1)

    ahead = steps <= 4 and narrow % 32 == 16 and hid_ref.shape[1] % (GROUP * narrow) == 0
    last_block = jnp.where(q * 2 < steps, steps - 1, 0)

    def prepare(sets):
        if not ahead:
            return
        at = token_lanes(sets)
        tiles, half_rows = pl.ds(0, lay.plain), pl.ds(lay.plain, LANE // 2)
        for n in range(1, steps):
            block = lax.rem(last_block + n, steps)
            hidden = hidden_block(block, sets)
            tile = product(tile_features(edge, lay.plain, block), hidden)
            half = product(half_features(block), hidden)
            ahead_ref[tiles, at] = tile if n == 1 else ahead_ref[tiles, at] + tile
            ahead_ref[half_rows, at] = half if n == 1 else ahead_ref[half_rows, at] + half

    def end_student(sets, take, begin, size):
        if not ahead:
            return product(take(), hidden_of(sets))
        return ahead_ref[pl.ds(begin, size), token_lanes(sets)] + product(take(last_block), hidden_block(last_block, sets))

    def rows_at(t):
        return pl.ds(pl.multiple_of(t * CHUNK, CHUNK), CHUNK)

    hop(far, span(0))
    own_body.wait()

    @pl.when(has_head)
    def _():
        own_head.wait()

    @pl.when(has_tail)
    def _():
        own_tail.wait()

    own_hid.wait()
    own_piece.wait()
    own_half.wait()
    for n in range(2):
        spread_all(n).wait_recv()
    teach_zero.wait_recv()

    @pl.when(has_head)
    def _():
        teach_head.wait_recv()

    main(features(0), rows_at(0), (jnp.where(has_head, 0, shift), CHUNK))

    def kept_chunk(t):
        hop(far, span(t))
        teach(t).wait_recv()
        main(features(t), rows_at(t))

    loop(1, kept, kept_chunk)

    @pl.when(server)
    def _():
        for n in range(2, 4):
            spread_all(n).wait_recv()

    @pl.when(~end)
    def _():
        def rest_chunk(t):
            hop(far, span(t))

            teach(t).wait_recv()
            main(features(t), rows_at(t))

            @pl.when(server)
            def _():
                extra_arrived(*extra_at(t)).wait_recv()
                more(features(t), rows_at(t - kept))

        loop(kept, whole - 1, rest_chunk)

        @pl.when(server)
        def _():
            prepare(tuple(range(2 * GROUP)))

        @pl.when(~server)
        def _():
            prepare(tuple(range(GROUP)))

        rest_chunk(whole - 1)

    def close(sets):
        at = pl.ds(sets[0] * tokens, len(sets) * tokens)
        values = gather_terms([acc[k, :, at] for k in range(5)])
        for n in range(len(sets)):
            stats_ref[sets[n]] = fold([value[:, n * tokens : (n + 1) * tokens] for value in values])

    def tell(n, sem, device, source_set):
        return remote(stats_ref.at[source_set], held_ref.at[n], stats_send.at[sem], stats_recv.at[sem], device)

    def told(sem, begin, size):
        at = held_ref.at[pl.ds(begin, size)]
        return remote(at, at, stats_send.at[sem], stats_recv.at[sem], (pr, c, d))

    limit = (0, lay.last + lay.shift * d - lay.stride)
    own_sets, all_sets = tuple(range(GROUP)), tuple(range(2 * GROUP))

    def tell_near():
        for n, (a, b, e, dj) in reversed(list(enumerate(peers))):
            tell(n, 0, (a, b, e), dj).start()

    def finish(sets):
        at = token_lanes(sets)

        def tile_terms(i):
            cut = tile_span(i)
            hop(far, cut)
            take = functools.partial(tile_features, cut[0], LANE)
            student = end_student(sets, take, pl.multiple_of(i * LANE, LANE), LANE)
            add_terms(student, acc, at, teacher_of(sets, cut[0], LANE))

        loop(0, lay.tiles, tile_terms)
        hop(far, half_span)

        @pl.when(half_used)
        def _():
            student = end_student(sets, half_features, lay.plain, LANE // 2)
            add_terms(student, acc, at, teacher_of(sets, lay.stride, LANE // 2), limit)

        close(sets)

    @pl.when(~end)
    def _():
        teach_end_arrived()

    @pl.when(server)
    def _():
        extra_arrived(*extra_body).wait_recv()

        @pl.when(has_tail)
        def _():
            extra_arrived(*extra_tail).wait_recv()

        finish(all_sets)
        for n, (a, b, e, dj) in reversed(list(enumerate(group))):
            tell(near + n, 1, (a - inward, b, e), GROUP + dj).start()

    @pl.when(~end & ~server)
    def _():
        finish(own_sets)

    @pl.when(end)
    def _():
        close(own_sets)

    tell_near()

    @pl.when(~end)
    def _():
        kinds = lax.broadcasted_iota(jnp.int32, held_ref.shape[1:], 0) % 2
        for n in range(len(group)):
            held_ref[near + n] = jnp.where(kinds == 0, LOW, 0.0)

    def settle(block):
        def sent(right, size):
            at = block_at(block, (0, size, 0, narrow))
            remote(at, at, (right_send if right else left_send).at[block, 0], line_recv.at[0, 0], (pr, c, d)).wait_send()

        def sent_half(right):
            at = block_at(block, half_span)
            remote(at, at, (right_send if right else left_send).at[block, 1], line_recv.at[0, 0], (pr, c, d)).wait_send()

        @pl.when((block <= q) & (q + 2 < steps))
        def _():
            sent(True, lay.stride)

            @pl.when(half_used)
            def _():
                sent_half(True)

        @pl.when((block <= q) & (q + 2 == steps))
        def _():
            sent(True, base)

        @pl.when((block >= q) & (q > 1))
        def _():
            sent(False, lay.stride)

            @pl.when(half_used)
            def _():
                sent_half(False)

        @pl.when((block >= q) & (q == 1))
        def _():
            sent(False, base)

    loop(0, steps, settle)
    sent_pieces = full_ref.at[0, pl.ds(0, count - 1)]
    remote(sent_pieces, sent_pieces, first_send.at[0], first_recv.at[0], (pr, c, d)).wait_send()

    def halves_sent(number):
        at = half_ref.at[0, pl.ds(0, number)]
        remote(at, at, first_send.at[1], first_recv.at[0], (pr, c, d)).wait_send()

    @pl.when(half_used)
    def _():
        halves_sent(depths - 1)

    @pl.when(~half_used)
    def _():
        halves_sent(depths)

    cross[0].wait_send()
    for n in range(2):
        spread_all(n).wait_send()
    taught = other_ref.at[pl.ds(shift, lay.last - shift)]
    remote(taught, taught, teach_send.at[0], teach_recv.at[0], (pr, c, d)).wait_send()

    @pl.when(peer_head)
    def _():
        teach_head.wait_send()

    @pl.when(peer_tail)
    def _():
        teach_tail.wait_send()

    @pl.when(end)
    def _():
        far_hid.wait_send()
        extra_arrived(0, base, lay.last - base).wait_send()

        @pl.when(has_tail)
        def _():
            extra_arrived(*extra_tail).wait_send()

    @pl.when(server)
    def _():
        cross[2].wait_send()
        for n in range(2, 4):
            spread_all(n).wait_send()
        told(1, near, len(group)).wait_send()

    told(0, 0, near).wait()

    @pl.when(end)
    def _():
        told(1, near, len(group)).wait_recv()

    blocks = [stats_ref[0]] + [held_ref[n] for n in range(near + len(group))]
    top = functools.reduce(jnp.maximum, blocks)
    scales = [jnp.exp(block - top) for block in blocks]
    weight = functools.reduce(jnp.add, scales)
    scaled = functools.reduce(jnp.add, [block * pltpu.roll(scale, 1, 0) for block, scale in zip(blocks, scales)])
    row_kind = lax.broadcasted_iota(jnp.int32, top.shape, 0) % 4
    sums_ref[...] = jnp.where(row_kind == 0, top, jnp.where(row_kind == 2, weight, scaled))


def on_device(rows, cols, depths, student_hidden, embedding, teacher_logits):
    vocab, narrow = embedding.shape
    lay = Layout(vocab, depths)
    hidden = student_hidden.T
    features, tokens = hidden.shape
    steps = rows // GROUP
    slots = 2 * GROUP * cols * depths - 1
    whole, height = lay.whole, lay.edge + lay.rest
    dma = pltpu.SemaphoreType.DMA
    any_space = pl.BlockSpec(memory_space=pl.ANY)
    dtype = embedding.dtype
    sums = pl.pallas_call(
        functools.partial(kernel, rows, cols, depths, lay),
        out_shape=jax.ShapeDtypeStruct((8, tokens // 2), jnp.float32),
        in_specs=[any_space] * 3,
        out_specs=pl.BlockSpec(memory_space=pltpu.VMEM),
        scratch_shapes=[
            pltpu.VMEM((narrow, vocab), dtype),
            pltpu.VMEM((depths * GROUP, narrow // 2, LANE), dtype),
            pltpu.VMEM((depths, rows, narrow, lay.stride), dtype),
            pltpu.VMEM((depths, rows, narrow // 2, LANE), dtype),
            pltpu.VMEM((height, tokens), teacher_logits.dtype),
            pltpu.VMEM((height, tokens), teacher_logits.dtype),
            pltpu.VMEM((GROUP, height - lay.kept * CHUNK, tokens), teacher_logits.dtype),
            pltpu.VMEM((depths * cols, features, 2 * GROUP * tokens), hidden.dtype),
            pltpu.VMEM((5, 8, 2 * GROUP * tokens), jnp.float32),
            pltpu.VMEM((lay.rest, 2 * GROUP * tokens), jnp.float32),
            pltpu.VMEM((2 * GROUP, 8, tokens // 2), jnp.float32),
            pltpu.VMEM((slots, 8, tokens // 2), jnp.float32),
            dma((7,)), dma((2,)), dma((whole + lay.tiles + 1,)), dma((steps, 2)), dma((steps, 2)), dma((steps - 1, whole + lay.tiles + 1)),
            dma((3,)), dma((whole + 3,)), dma((2,)), dma((whole - lay.kept + 2,)),
            dma((3 + 2 * GROUP,)), dma((3 + 2 * GROUP,)), dma((2,)), dma((2,)),
        ],
        compiler_params=pltpu.CompilerParams(collective_id=0, has_side_effects=True, vmem_limit_bytes=54 * 2**20 - 84 * 2**10),
        name="distill",
    )(embedding.T, teacher_logits.T, hidden)
    peak, total, weight, cross = (sums.reshape(2, 4, -1)[:, k].reshape(-1) for k in range(4))
    norm_log = jnp.log(total)
    return peak + norm_log - cross / weight, -norm_log


def solution(mesh):
    sizes = [mesh.shape[name] for name in ("row", "col", "depth")]
    in_specs = (P("row", ("depth", "col")), P("col", ("depth", "row")), P("row", ("col", "depth")))
    out_specs = (P("row"), P("row"))
    return jax.shard_map(
        functools.partial(on_device, *sizes), mesh=mesh, in_specs=in_specs, out_specs=out_specs, check_vma=False
    )
```

```python
import functools

import jax
import jax.numpy as jnp
from jax import lax
from jax.experimental import pallas as pl
from jax.experimental.pallas import tpu as pltpu
from jax.sharding import PartitionSpec as P

MESH = pl.DeviceIdType.MESH
GROUP = 2
LANE = 128
CHUNK = 384
KEPT = 0.67
LOW = -1e30


class Layout:
    def __init__(self, vocab, depths):
        self.half = vocab // depths
        self.stride = vocab // LANE // (depths * GROUP) * LANE
        self.shift = self.half - GROUP * self.stride
        self.last = self.half - (GROUP - 1) * self.stride
        self.edge = ((self.stride - LANE) // CHUNK - 2) * CHUNK
        self.whole = self.edge // CHUNK
        self.plain = self.stride - self.edge
        self.tiles = self.plain // LANE
        self.rest = self.plain + LANE // 2
        self.kept = round(self.stride / CHUNK * KEPT)
        assert depths == 2 and GROUP == 2 and 0 <= self.shift < CHUNK and self.shift % 16 == 0
        assert self.last + self.shift <= self.stride + LANE // 2 and self.plain % LANE == 0
        assert vocab <= self.stride * depths * GROUP + LANE // 2


def place():
    r, c, d = lax.axis_index("row"), lax.axis_index("col"), lax.axis_index("depth")
    return r, c, d, r // GROUP, lax.rem(r, GROUP)


def ends(rows, q):
    steps = rows // GROUP
    low, high = q == 0, q == steps - 1
    return low | high, (q == 1) | (q == steps - 2), jnp.where(q * 2 < steps, GROUP, -GROUP)


def as_count(flag):
    return flag.astype(jnp.int32)


def loop(begin, stop, body):
    def step(i, _):
        body(i)
        return 0

    lax.fori_loop(begin, stop, step, 0)


def gather_terms(parts):
    top, total, teacher_top, teacher_total, cross = parts
    peak = jnp.max(top, axis=0, keepdims=True)
    teacher_peak = jnp.max(teacher_top, axis=0, keepdims=True)
    scale = jnp.exp(teacher_top - teacher_peak)
    weight = jnp.sum(teacher_total * scale, axis=0, keepdims=True)
    return [
        peak,
        jnp.sum(total * jnp.exp(top - peak), axis=0, keepdims=True),
        teacher_peak + jnp.log(weight),
        jnp.sum(cross * scale, axis=0, keepdims=True) / weight,
    ]


def fold(values):
    whole = jnp.concatenate(values, axis=0)
    half = whole.shape[1] // 2
    return jnp.concatenate([whole[:, :half], whole[:, half:]], axis=0)


def product(rows, hidden):
    return lax.dot_general(rows, hidden, (((0,), (0,)), ((), ())), preferred_element_type=jnp.float32)


def add_terms(student, acc, at, teacher, valid=None):
    size = student.shape[0]
    teacher = teacher.astype(jnp.float32)
    if valid is not None:
        index = lax.broadcasted_iota(jnp.int32, student.shape, 0)
        keep = (index >= valid[0]) & (index < valid[1])
        student = jnp.where(keep, student, LOW)
        teacher = jnp.where(keep, teacher, LOW)
    student = student.reshape(size // 8, 8, -1)
    teacher = teacher.reshape(size // 8, 8, -1)
    old, teacher_old = acc[0, :, at], acc[2, :, at]
    top = jnp.maximum(old, jnp.max(student, axis=0))
    acc[1, :, at] = acc[1, :, at] * jnp.exp(old - top) + jnp.sum(jnp.exp(student - top[None]), axis=0)
    acc[0, :, at] = top
    teacher_top = jnp.maximum(teacher_old, jnp.max(teacher, axis=0))
    fade = jnp.exp(teacher_old - teacher_top)
    weights = jnp.exp(teacher - teacher_top[None])
    acc[3, :, at] = acc[3, :, at] * fade + jnp.sum(weights, axis=0)
    acc[4, :, at] = acc[4, :, at] * fade + jnp.sum(weights * student, axis=0)
    acc[2, :, at] = teacher_top


def kernel(
    rows, cols, depths, lay, emb_ref, teacher_ref, hidden_ref, sums_ref,
    table_ref, pack_ref, full_ref, half_ref, own_ref, other_ref, extra_ref, hid_ref, acc, ahead_ref, stats_ref, held_ref,
    own_sem, first_send, first_recv, right_send, left_send, line_recv, teach_send, teach_recv, extra_send, extra_recv,
    hid_send, hid_recv, stats_send, stats_recv,
):
    r, c, d, q, j = place()
    steps = rows // GROUP
    count = depths * GROUP
    me = d * GROUP + j
    kept, whole, edge = lay.kept, lay.whole, lay.edge
    narrow = table_ref.shape[0]
    packed = narrow // 2
    tokens = hidden_ref.shape[1]
    end, server, inward = ends(rows, q)
    pj = lax.rem(j + 1, GROUP)
    pr = q * GROUP + pj
    slice_ = d * cols + c
    peers = []
    for dj in range(GROUP):
        for dc in range(cols):
            for dd in range(depths):
                if dj or dc or dd:
                    peers.append((q * GROUP + lax.rem(j + dj, GROUP), lax.rem(c + dc, cols), lax.rem(d + dd, depths), dj))
    group = [(r, c, d, 0)] + peers
    near = len(peers)
    same = [(a, b, e) for a, b, e, dj in peers if dj == 0]

    barrier = pltpu.get_barrier_semaphore()

    def greet(row, col, depth):
        pl.semaphore_signal(barrier, inc=1, device_id=(row, col, depth), device_id_type=MESH)

    @pl.when(q + 1 < steps)
    def _():
        greet(r + GROUP, c, d)

    @pl.when(q > 0)
    def _():
        greet(r - GROUP, c, d)

    greet(pr, c, d)
    greet(r, lax.rem(c + 1, cols), d)
    greet(r, c, lax.rem(d + 1, depths))

    def remote(source_ref, dst_ref, send_sem, recv_sem, device):
        return pltpu.make_async_remote_copy(
            src_ref=source_ref, dst_ref=dst_ref, send_sem=send_sem, recv_sem=recv_sem, device_id=device, device_id_type=MESH
        )

    load = pltpu.make_async_copy(emb_ref, table_ref, own_sem.at[0])
    strip = 8 if narrow % 8 == 0 else narrow
    for at in range(0, narrow, strip):
        rows_ = pl.ds(at, strip)
        pltpu.make_async_copy(emb_ref.at[rows_], table_ref.at[rows_], own_sem.at[0]).start()
    load.wait()
    for target in range(count):
        part = table_ref[:, lay.stride * (target + 1) : lay.stride * (target + 1) + LANE // 2]
        pack_ref[target] = jnp.concatenate([part[:packed], part[packed:]], axis=1)

    def span(t):
        return pl.multiple_of(t * CHUNK, CHUNK), CHUNK, t, narrow

    def tile_span(i):
        return pl.multiple_of(edge + i * LANE, LANE), LANE, whole + i, narrow

    half_span = (lay.stride, LANE, whole + lay.tiles, packed)
    ends_of = tuple(tile_span(i) for i in range(lay.tiles)) + (half_span,)

    def piece(target, cut):
        first_lane, size, index, height = cut
        if height != narrow:
            return pack_ref.at[target]
        return table_ref.at[:, pl.ds(pl.multiple_of(lay.stride * target + first_lane, LANE), size)]

    def slot(depth, row, cut):
        first_lane, size, _, height = cut
        return full_ref.at[depth, row, :, pl.ds(first_lane, size)] if height == narrow else half_ref.at[depth, row]

    def block_at(block, cut):
        first_lane, size, _, height = cut
        row = pl.ds(pl.multiple_of(block * GROUP, GROUP), GROUP)
        return full_ref.at[:, row, :, pl.ds(first_lane, size)] if height == narrow else half_ref.at[:, row]

    own_piece = pltpu.make_async_copy(
        table_ref.at[:, pl.ds(pl.multiple_of(lay.stride * me, LANE), lay.stride)],
        full_ref.at[d, r], own_sem.at[1],
    )
    own_half = pltpu.make_async_copy(pack_ref.at[me], slot(d, r, half_span), own_sem.at[2])

    def kind(cut):
        return 0 if cut[3] == narrow else 1

    def first(cut, off):
        target = lax.rem(me + off, count)
        return remote(
            piece(target, cut), slot(d, r, cut), first_send.at[kind(cut)], first_recv.at[cut[2]],
            (q * GROUP + lax.rem(target, GROUP), c, target // GROUP),
        )

    def first_arrived(cut):
        row = pl.ds(0, count - 1)
        at = full_ref.at[0, row, :, pl.ds(cut[0], cut[1])] if cut[3] == narrow else half_ref.at[0, row]
        return remote(at, at, first_send.at[0], first_recv.at[cut[2]], (pr, c, d))

    def send_line(source_ref, dst_ref, block, cut, right):
        sems, place_ = (right_send, block) if right else (left_send, block - 1)
        return remote(
            source_ref, dst_ref, sems.at[block, kind(cut)], line_recv.at[place_, cut[2]],
            (r + GROUP if right else r - GROUP, c, d),
        )

    def along(block, cut, right):
        at = block_at(block, cut)
        return send_line(at, at, block, cut, right)

    def arrived(block, cut, right):
        at = block_at(block, cut)
        return remote(at, at, right_send.at[0, 0], line_recv.at[block if right else block - 1, cut[2]], (pr, c, d))

    half_used = j == GROUP - 1

    def uses(cut, flag):
        return flag if cut[3] == narrow else flag & half_used

    def to_right(t):
        return (q + 1 < steps) & ((t < kept) | (q + 2 < steps))

    def to_left(t):
        return (q > 0) & ((t < kept) | (q > 1))

    def both(cut, source_ref, dst_ref):
        @pl.when(uses(cut, to_right(cut[2])))
        def _():
            send_line(source_ref, dst_ref, q, cut, True).start()

        @pl.when(uses(cut, to_left(cut[2])))
        def _():
            send_line(source_ref, dst_ref, q, cut, False).start()

    def hidden_at(n, where=None):
        return hid_ref.at[slice_ if where is None else where, :, pl.ds(n * tokens, tokens)]

    def give(n, sem, device, source_ref):
        return remote(source_ref, hidden_at(n), hid_send.at[sem], hid_recv.at[sem], device)

    cross = [give(1, 0, (pr, c, d), hidden_ref), None, give(3, 1, (pr, c, d), hidden_at(2))]
    far_hid = give(2, 2, (r + inward, c, d), hidden_ref)
    spread = [
        [give(n, 3 + n, device, hidden_ref if n == 0 else hidden_at(n)) for device in same] for n in range(2 * GROUP)
    ]

    def spread_all(n):
        at = hidden_at(n, pl.ds(0, len(same)))
        return remote(at, at, hid_send.at[3 + n], hid_recv.at[3 + n], (pr, c, d))

    pl.semaphore_wait(barrier, 3 + as_count(q + 1 < steps) + as_count(q > 0))

    @pl.when(end)
    def _():
        far_hid.start()

    cross[0].start()
    by_x, by_y, by_both = GROUP, jnp.where(j == 0, 1, count - 1), jnp.where(j == 0, count - 1, 1)

    def launch_own(cut):
        both(cut, piece(me, cut), slot(d, r, cut))

    def launch_first(cut, off, ahead_):
        if cut[3] == narrow:
            first(cut, off).start()
            return

        @pl.when(half_used == ahead_)
        def _():
            first(cut, off).start()

    def launch_near(cut):
        launch_first(cut, by_y, False)
        launch_first(cut, by_x, True)

    def launch_far(cut):
        launch_first(cut, by_both, False)

    def opening(t):
        launch_own(span(t))
        launch_near(span(t))

    lead = min(4, whole)
    loop(0, lead, opening)
    loop(lead, whole, lambda t: launch_own(span(t)))
    for cut in ends_of:
        launch_own(cut)
    cross[0].wait_recv()

    def crossing(t):
        launch_far(span(t - lead))
        launch_near(span(t))

    loop(lead, whole, crossing)
    loop(whole - lead, whole, lambda t: launch_far(span(t)))
    for cut in ends_of:
        launch_near(cut)
        launch_far(cut)

    has_head = ~((d > 0) & (j == 0))
    peer_head = ~((d > 0) & (pj == 0))
    has_tail = (d == depths - 1) & (j == GROUP - 1)
    peer_tail = (d == depths - 1) & (pj == GROUP - 1)
    shift = lay.shift * (depths - 1)

    def source(part, at, size):
        begin = jnp.clip(lay.stride * part - lay.shift * d + at, 0, lay.half - size)
        return teacher_ref.at[pl.ds(pl.multiple_of(begin, 16), size)]

    own_body = pltpu.make_async_copy(source(j, shift, lay.last - shift), own_ref.at[pl.ds(shift, lay.last - shift)], own_sem.at[3])
    own_head = pltpu.make_async_copy(source(j, 0, shift), own_ref.at[pl.ds(0, shift)], own_sem.at[4])
    own_tail = pltpu.make_async_copy(source(j, lay.last, shift), own_ref.at[pl.ds(lay.last, shift)], own_sem.at[5])
    own_hid = pltpu.make_async_copy(hidden_ref, hidden_at(0), own_sem.at[6])
    own_piece.start()
    own_half.start()
    own_hid.start()
    own_body.start()

    @pl.when(has_head)
    def _():
        own_head.start()

    @pl.when(has_tail)
    def _():
        own_tail.start()

    @pl.when(server)
    def _():
        far_hid.wait_recv()
        cross[2].start()

    def start_line(cut):
        first_arrived(cut).wait_recv()
        for off in range(1, count):
            sender = lax.rem(me + count - off, count)
            at = slot(sender // GROUP, q * GROUP + lax.rem(sender, GROUP), cut)
            both(cut, at, at)


    body = lay.last - edge

    def teach_rows(index, at, size, sem=0):
        return remote(source(pj, at, size), other_ref.at[pl.ds(at, size)], teach_send.at[sem], teach_recv.at[index], (pr, c, d))

    def teach(t):
        return teach_rows(t, pl.multiple_of(t * CHUNK, CHUNK), CHUNK)

    teach_zero = teach_rows(0, shift, CHUNK - shift)
    teach_head = teach_rows(whole + 1, 0, shift, 1)
    teach_body = teach_rows(whole, edge, body)
    teach_tail = teach_rows(whole + 2, lay.last, shift, 2)

    def teach_kept():
        teach_zero.start()

        @pl.when(peer_head)
        def _():
            teach_head.start()

        loop(1, kept, lambda t: teach(t).start())

    def teach_rest():
        loop(kept, whole, lambda t: teach(t).start())
        teach_body.start()

        @pl.when(peer_tail)
        def _():
            teach_tail.start()

    loop(0, whole * 3 // 4, lambda t: start_line(span(t)))

    @pl.when(end)
    def _():
        teach_rest()

    teach_kept()

    @pl.when(~end)
    def _():
        teach_rest()

    loop(whole * 3 // 4, whole, lambda t: start_line(span(t)))
    for cut in ends_of[:-1]:
        start_line(cut)

    @pl.when(half_used)
    def _():
        start_line(half_span)

    for copy in spread[0] + spread[1]:
        copy.start()

    @pl.when(server)
    def _():
        cross[2].wait_recv()
        for copy in spread[2] + spread[3]:
            copy.start()

    def teach_end_arrived():
        teach_body.wait_recv()

        @pl.when(has_tail)
        def _():
            teach_tail.wait_recv()

    base = kept * CHUNK

    def extra_rows(n, index, at, size, sem=0):
        return remote(
            source(j, at, size) if n == 0 else other_ref.at[pl.ds(at, size)],
            extra_ref.at[n, pl.ds(at - base, size)], extra_send.at[sem], extra_recv.at[index], (r + inward, c, d),
        )

    def extra_arrived(index, at, size, sem=0):
        both_sets = extra_ref.at[:, pl.ds(at - base, size)]
        return remote(both_sets, both_sets, extra_send.at[sem], extra_recv.at[index], (pr, c, d))

    def extra_at(t):
        return t - kept, pl.multiple_of(t * CHUNK, CHUNK), CHUNK

    extra_body = (whole - kept, edge, body)
    extra_tail = (whole - kept + 1, lay.last, shift, 1)

    @pl.when(end)
    def _():
        def pass_on(t):
            teach(t).wait_recv()
            for n in range(GROUP):
                extra_rows(n, *extra_at(t)).start()

        loop(kept, whole, pass_on)
        teach_end_arrived()
        for n in range(GROUP):
            extra_rows(n, *extra_body).start()

        @pl.when(has_tail)
        def _():
            for n in range(GROUP):
                extra_rows(n, *extra_tail).start()

    def hop(k, cut):
        t = cut[2]
        wanted = uses(cut, (t < kept) | ~end)

        @pl.when((q - k >= 0) & wanted)
        def _():
            arrived(q - k, cut, True).wait_recv()

            @pl.when(to_right(t))
            def _():
                along(q - k, cut, True).start()

        @pl.when((q + k < steps) & wanted)
        def _():
            arrived(q + k, cut, False).wait_recv()

            @pl.when(to_left(t))
            def _():
                along(q + k, cut, False).start()

    far = jnp.maximum(q, steps - 1 - q)

    def early(k):
        loop(0, whole, lambda t: hop(k, span(t)))
        for cut in ends_of:
            hop(k, cut)

    loop(1, far, early)

    for k in range(5):
        acc[k] = jnp.full(acc.shape[1:], LOW if k in (0, 2) else 0.0, jnp.float32)

    def features(t):
        return full_ref[:, :, :, pl.ds(pl.multiple_of(t * CHUNK, CHUNK), CHUNK)].reshape(-1, CHUNK)

    def token_lanes(sets):
        return pl.ds(sets[0] * tokens, len(sets) * tokens)

    def hidden_of(sets):
        return hid_ref[:, :, token_lanes(sets)].reshape(-1, len(sets) * tokens)

    def unpacked(half):
        half = jnp.concatenate([half[..., : LANE // 2], half[..., LANE // 2 :]], axis=2)
        return half.reshape(-1, LANE // 2)

    def tile_features(begin, size, block=None):
        at = pl.ds(0, rows) if block is None else pl.ds(block * GROUP, GROUP)
        return full_ref[:, at, :, pl.ds(begin, size)].reshape(-1, size)

    def half_features(block=None):
        return unpacked(half_ref[:, pl.ds(0, rows) if block is None else pl.ds(block * GROUP, GROUP)])

    def hidden_block(block, sets):
        begin = block * (GROUP * narrow)
        at = pl.ds(pl.multiple_of(lax.rem(begin, hid_ref.shape[1]), 16), GROUP * narrow)
        parts = [hid_ref[depth * cols + begin // hid_ref.shape[1], at, token_lanes(sets)] for depth in range(depths)]
        return jnp.concatenate(parts, axis=0)

    def main(rows_, at, valid=None):
        for n, ref in enumerate((own_ref, other_ref)):
            add_terms(product(rows_, hidden_of((n,))), acc, token_lanes((n,)), ref[at, :], valid)

    def more(rows_, at):
        for n in range(GROUP):
            add_terms(product(rows_, hidden_of((GROUP + n,))), acc, token_lanes((GROUP + n,)), extra_ref[n, at, :])

    def teacher_of(sets, begin, size):
        at = pl.ds(begin, size)
        own = [own_ref[at, :], other_ref[at, :]]
        taken = [extra_ref[n, pl.ds(pl.multiple_of(begin - base, LANE // 2), size), :] for n in range(GROUP)] if len(sets) > GROUP else []
        return jnp.concatenate(own + taken, axis=1)

    ahead = steps <= 4 and narrow % 32 == 16 and hid_ref.shape[1] % (GROUP * narrow) == 0
    last_block = jnp.where(q * 2 < steps, steps - 1, 0)

    def prepare(sets):
        if not ahead:
            return
        at = token_lanes(sets)
        tiles, half_rows = pl.ds(0, lay.plain), pl.ds(lay.plain, LANE // 2)
        for n in range(1, steps):
            block = lax.rem(last_block + n, steps)
            hidden = hidden_block(block, sets)
            tile = product(tile_features(edge, lay.plain, block), hidden)
            half = product(half_features(block), hidden)
            ahead_ref[tiles, at] = tile if n == 1 else ahead_ref[tiles, at] + tile
            ahead_ref[half_rows, at] = half if n == 1 else ahead_ref[half_rows, at] + half

    def end_student(sets, take, begin, size):
        if not ahead:
            return product(take(), hidden_of(sets))
        return ahead_ref[pl.ds(begin, size), token_lanes(sets)] + product(take(last_block), hidden_block(last_block, sets))

    def rows_at(t):
        return pl.ds(pl.multiple_of(t * CHUNK, CHUNK), CHUNK)

    hop(far, span(0))
    own_body.wait()

    @pl.when(has_head)
    def _():
        own_head.wait()

    @pl.when(has_tail)
    def _():
        own_tail.wait()

    own_hid.wait()
    own_piece.wait()
    own_half.wait()
    for n in range(2):
        spread_all(n).wait_recv()
    teach_zero.wait_recv()

    @pl.when(has_head)
    def _():
        teach_head.wait_recv()

    main(features(0), rows_at(0), (jnp.where(has_head, 0, shift), CHUNK))

    def kept_chunk(t):
        hop(far, span(t))
        teach(t).wait_recv()
        main(features(t), rows_at(t))

    loop(1, kept, kept_chunk)

    @pl.when(server)
    def _():
        for n in range(2, 4):
            spread_all(n).wait_recv()

    @pl.when(~end)
    def _():
        def rest_chunk(t):
            hop(far, span(t))

            teach(t).wait_recv()
            main(features(t), rows_at(t))

            @pl.when(server)
            def _():
                extra_arrived(*extra_at(t)).wait_recv()
                more(features(t), rows_at(t - kept))

        loop(kept, whole - 1, rest_chunk)

        @pl.when(server)
        def _():
            prepare(tuple(range(2 * GROUP)))

        @pl.when(~server)
        def _():
            prepare(tuple(range(GROUP)))

        rest_chunk(whole - 1)

    def close(sets):
        at = pl.ds(sets[0] * tokens, len(sets) * tokens)
        values = gather_terms([acc[k, :, at] for k in range(5)])
        for n in range(len(sets)):
            stats_ref[sets[n]] = fold([value[:, n * tokens : (n + 1) * tokens] for value in values])

    def tell(n, sem, device, source_set):
        return remote(stats_ref.at[source_set], held_ref.at[n], stats_send.at[sem], stats_recv.at[sem], device)

    def told(sem, begin, size):
        at = held_ref.at[pl.ds(begin, size)]
        return remote(at, at, stats_send.at[sem], stats_recv.at[sem], (pr, c, d))

    limit = (0, lay.last + lay.shift * d - lay.stride)
    own_sets, all_sets = tuple(range(GROUP)), tuple(range(2 * GROUP))

    def tell_near():
        for n, (a, b, e, dj) in reversed(list(enumerate(peers))):
            tell(n, 0, (a, b, e), dj).start()

    def finish(sets):
        at = token_lanes(sets)

        def tile_terms(i):
            cut = tile_span(i)
            hop(far, cut)
            take = functools.partial(tile_features, cut[0], LANE)
            student = end_student(sets, take, pl.multiple_of(i * LANE, LANE), LANE)
            add_terms(student, acc, at, teacher_of(sets, cut[0], LANE))

        loop(0, lay.tiles, tile_terms)
        hop(far, half_span)

        @pl.when(half_used)
        def _():
            student = end_student(sets, half_features, lay.plain, LANE // 2)
            add_terms(student, acc, at, teacher_of(sets, lay.stride, LANE // 2), limit)

        close(sets)

    @pl.when(~end)
    def _():
        teach_end_arrived()

    @pl.when(server)
    def _():
        extra_arrived(*extra_body).wait_recv()

        @pl.when(has_tail)
        def _():
            extra_arrived(*extra_tail).wait_recv()

        finish(all_sets)
        for n, (a, b, e, dj) in reversed(list(enumerate(group))):
            tell(near + n, 1, (a - inward, b, e), GROUP + dj).start()

    @pl.when(~end & ~server)
    def _():
        finish(own_sets)

    @pl.when(end)
    def _():
        close(own_sets)

    tell_near()

    @pl.when(~end)
    def _():
        kinds = lax.broadcasted_iota(jnp.int32, held_ref.shape[1:], 0) % 2
        for n in range(len(group)):
            held_ref[near + n] = jnp.where(kinds == 0, LOW, 0.0)

    def settle(block):
        def sent(right, size):
            at = block_at(block, (0, size, 0, narrow))
            remote(at, at, (right_send if right else left_send).at[block, 0], line_recv.at[0, 0], (pr, c, d)).wait_send()

        def sent_half(right):
            at = block_at(block, half_span)
            remote(at, at, (right_send if right else left_send).at[block, 1], line_recv.at[0, 0], (pr, c, d)).wait_send()

        @pl.when((block <= q) & (q + 2 < steps))
        def _():
            sent(True, lay.stride)

            @pl.when(half_used)
            def _():
                sent_half(True)

        @pl.when((block <= q) & (q + 2 == steps))
        def _():
            sent(True, base)

        @pl.when((block >= q) & (q > 1))
        def _():
            sent(False, lay.stride)

            @pl.when(half_used)
            def _():
                sent_half(False)

        @pl.when((block >= q) & (q == 1))
        def _():
            sent(False, base)

    loop(0, steps, settle)
    sent_pieces = full_ref.at[0, pl.ds(0, count - 1)]
    remote(sent_pieces, sent_pieces, first_send.at[0], first_recv.at[0], (pr, c, d)).wait_send()

    def halves_sent(number):
        at = half_ref.at[0, pl.ds(0, number)]
        remote(at, at, first_send.at[1], first_recv.at[0], (pr, c, d)).wait_send()

    @pl.when(half_used)
    def _():
        halves_sent(depths - 1)

    @pl.when(~half_used)
    def _():
        halves_sent(depths)

    cross[0].wait_send()
    for n in range(2):
        spread_all(n).wait_send()
    taught = other_ref.at[pl.ds(shift, lay.last - shift)]
    remote(taught, taught, teach_send.at[0], teach_recv.at[0], (pr, c, d)).wait_send()

    @pl.when(peer_head)
    def _():
        teach_head.wait_send()

    @pl.when(peer_tail)
    def _():
        teach_tail.wait_send()

    @pl.when(end)
    def _():
        far_hid.wait_send()
        extra_arrived(0, base, lay.last - base).wait_send()

        @pl.when(has_tail)
        def _():
            extra_arrived(*extra_tail).wait_send()

    @pl.when(server)
    def _():
        cross[2].wait_send()
        for n in range(2, 4):
            spread_all(n).wait_send()
        told(1, near, len(group)).wait_send()

    told(0, 0, near).wait()

    @pl.when(end)
    def _():
        told(1, near, len(group)).wait_recv()

    blocks = [stats_ref[0]] + [held_ref[n] for n in range(near + len(group))]
    top = functools.reduce(jnp.maximum, blocks)
    scales = [jnp.exp(block - top) for block in blocks]
    weight = functools.reduce(jnp.add, scales)
    scaled = functools.reduce(jnp.add, [block * pltpu.roll(scale, 1, 0) for block, scale in zip(blocks, scales)])
    row_kind = lax.broadcasted_iota(jnp.int32, top.shape, 0) % 4
    sums_ref[...] = jnp.where(row_kind == 0, top, jnp.where(row_kind == 2, weight, scaled))


def on_device(rows, cols, depths, student_hidden, embedding, teacher_logits):
    vocab, narrow = embedding.shape
    lay = Layout(vocab, depths)
    hidden = student_hidden.T
    features, tokens = hidden.shape
    steps = rows // GROUP
    slots = 2 * GROUP * cols * depths - 1
    whole, height = lay.whole, lay.edge + lay.rest
    dma = pltpu.SemaphoreType.DMA
    any_space = pl.BlockSpec(memory_space=pl.ANY)
    dtype = embedding.dtype
    sums = pl.pallas_call(
        functools.partial(kernel, rows, cols, depths, lay),
        out_shape=jax.ShapeDtypeStruct((8, tokens // 2), jnp.float32),
        in_specs=[any_space] * 3,
        out_specs=pl.BlockSpec(memory_space=pltpu.VMEM),
        scratch_shapes=[
            pltpu.VMEM((narrow, vocab), dtype),
            pltpu.VMEM((depths * GROUP, narrow // 2, LANE), dtype),
            pltpu.VMEM((depths, rows, narrow, lay.stride), dtype),
            pltpu.VMEM((depths, rows, narrow // 2, LANE), dtype),
            pltpu.VMEM((height, tokens), teacher_logits.dtype),
            pltpu.VMEM((height, tokens), teacher_logits.dtype),
            pltpu.VMEM((GROUP, height - lay.kept * CHUNK, tokens), teacher_logits.dtype),
            pltpu.VMEM((depths * cols, features, 2 * GROUP * tokens), hidden.dtype),
            pltpu.VMEM((5, 8, 2 * GROUP * tokens), jnp.float32),
            pltpu.VMEM((lay.rest, 2 * GROUP * tokens), jnp.float32),
            pltpu.VMEM((2 * GROUP, 8, tokens // 2), jnp.float32),
            pltpu.VMEM((slots, 8, tokens // 2), jnp.float32),
            dma((7,)), dma((2,)), dma((whole + lay.tiles + 1,)), dma((steps, 2)), dma((steps, 2)), dma((steps - 1, whole + lay.tiles + 1)),
            dma((3,)), dma((whole + 3,)), dma((2,)), dma((whole - lay.kept + 2,)),
            dma((3 + 2 * GROUP,)), dma((3 + 2 * GROUP,)), dma((2,)), dma((2,)),
        ],
        compiler_params=pltpu.CompilerParams(collective_id=0, has_side_effects=True, vmem_limit_bytes=54 * 2**20 - 84 * 2**10),
        name="distill",
    )(embedding.T, teacher_logits.T, hidden)
    peak, total, weight, cross = (sums.reshape(2, 4, -1)[:, k].reshape(-1) for k in range(4))
    norm_log = jnp.log(total)
    return peak + norm_log - cross / weight, -norm_log


def solution(mesh):
    sizes = [mesh.shape[name] for name in ("row", "col", "depth")]
    in_specs = (P("row", ("depth", "col")), P("col", ("depth", "row")), P("row", ("col", "depth")))
    out_specs = (P("row"), P("row"))
    return jax.shard_map(
        functools.partial(on_device, *sizes), mesh=mesh, in_specs=in_specs, out_specs=out_specs, check_vma=False
    )
```
